128 devices in a mesh: gz: 32 (over z, y, core), gy: 4 (over x).
Axes of the slice: x: 4, y: 4, z: 4, core: 2. Of those that a mesh axis runs over, the one named last changes fastest.
Arguments:
- right_side: float32 [8, 64, 256, 512], P(None, 'gz', 'gy'), may hold values from -8 to 8
- diagonal: float32 [64, 256, 512], P('gz', 'gy'), may hold values from 0.1 to 4
Outputs:
- solution: float32 [8, 64, 256, 512], P(None, 'gz', 'gy')
- hessenberg: float32 [24, 32], replicated
The draws below stay inside these ranges and needn't reach their ends.
All inputs are finite; a program needn't handle non-finite values.
Results may differ from the reference program's by a relative error of at most 0.0003.
Values sent between devices are 32-bit elements; how exact they have to be, the bound alone decides.
A program may use at most 64 MiB of HBM per device.

```python
import math
import jax
import jax.numpy as jnp
from jax import lax

BLK = 8
ITERS = 3
NX = 512
NZ = 64
NY = 256


def level_of(rng, dims, shards, smallest, top_value):
    gain = 1.0
    for axis_at, shards_of in shards:
        draws = jax.random.uniform(jax.random.fold_in(jax.random.fold_in(rng, 6), axis_at), (shards_of,), jnp.float32, smallest / len(shards), top_value / len(shards))
        gain = gain * jnp.repeat(jnp.exp(draws), dims[axis_at] // shards_of).reshape((-1,) + (1,) * (len(dims) - 1 - axis_at))
    return gain


def gaussian(key, shape, deviation, most, split=(), dtype=jnp.bfloat16):
    level = level_of(key, shape, split, -0.22, 0.18) if split else 1.0
    drawn = jax.random.normal(key, shape, jnp.float32) * deviation * level
    return jnp.minimum(jnp.maximum(drawn, -most), most).astype(dtype)


def setup_inputs(seed: int = 0) -> dict:
    streams_of = jax.random.split(jax.random.key(seed), 3)
    return {
        "right_side": gaussian(streams_of[0], (BLK, NZ, NY, NX), 1.0, 8.0, ((1, 32), (2, 4)), jnp.float32),
        "diagonal": jnp.clip(jnp.exp(math.log(4.0) - 3.6888794 * jax.random.uniform(streams_of[1], (NZ, NY, NX), jnp.float32) ** level_of(streams_of[1], (NZ, NY, NX), ((0, 32), (1, 4)), -0.2, 0.2)), 0.1, 4.0),
    }


def apply_op(field, diagonal):
    padded = jnp.pad(field, ((0, 0), (1, 1), (1, 1), (1, 1)))
    beside = padded[:, 2:, 1:-1, 1:-1] + padded[:, :-2, 1:-1, 1:-1]
    beside = beside + padded[:, 1:-1, 2:, 1:-1] + padded[:, 1:-1, :-2, 1:-1]
    beside = beside + padded[:, 1:-1, 1:-1, 2:] + padded[:, 1:-1, 1:-1, :-2]
    return (6.0 + diagonal)[None] * field - beside

def inner(left, right):
    return jnp.dot(left, right.T, precision=lax.Precision.HIGHEST)

def reference(right_side, diagonal):
    shape = right_side.shape
    flat_rhs = right_side.reshape(BLK, -1)
    lower0 = jnp.linalg.cholesky(inner(flat_rhs, flat_rhs))
    basis = [jax.scipy.linalg.solve_triangular(lower0, flat_rhs, lower=True)]
    blocks = []
    for step in range(ITERS):
        work = apply_op(basis[step].reshape(shape), diagonal).reshape(BLK, -1)
        coeff = [inner(work, vec) for vec in basis]
        reduced = work
        for index in range(step + 1):
            reduced = reduced - jnp.dot(coeff[index], basis[index], precision=lax.Precision.HIGHEST)
        lower = jnp.linalg.cholesky(inner(reduced, reduced))
        basis.append(jax.scipy.linalg.solve_triangular(lower, reduced, lower=True))
        row = coeff + [lower] + [jnp.zeros((BLK, BLK), jnp.float32)] * (ITERS - 1 - step)
        blocks.append(jnp.concatenate(row, axis=1))
    hessenberg = jnp.concatenate(blocks, axis=0)
    normal = jnp.dot(hessenberg, hessenberg.T, precision=lax.Precision.HIGHEST)
    factor = jnp.linalg.cholesky(normal)
    target = jnp.dot(hessenberg[:, :BLK], lower0.T, precision=lax.Precision.HIGHEST)
    coeffs = jax.scipy.linalg.cho_solve((factor, True), target)
    stacked = jnp.concatenate(basis[:ITERS], axis=0)
    solution = jnp.dot(coeffs.T, stacked, precision=lax.Precision.HIGHEST)
    return (solution.reshape(shape), hessenberg)
```

```python
import functools

import jax
import jax.numpy as jnp
from jax import lax
from jax.experimental import pallas as pl
from jax.experimental.pallas import tpu as pltpu
from jax.sharding import PartitionSpec as P

MESH = pl.DeviceIdType.MESH
BLK = 8
ITERS = 3
SHIFT = 7.0
TOP = 8
Y_CHIPS = 4
CORES = 2


def iotas():
    return (
        lax.broadcasted_iota(jnp.int32, (8, 128), 0),
        lax.broadcasted_iota(jnp.int32, (8, 128), 1),
    )


def sublane(tile, at):
    return jnp.broadcast_to(tile[at : at + 1, :], (8, 128))


def lane(tile, at):
    return jnp.broadcast_to(tile[:, at : at + 1], (8, 128))


def rsqrt(value):
    guess = lax.rsqrt(value)
    return guess * (1.5 - 0.5 * value * guess * guess)


def weights_of(moments):
    sub, _ = iotas()
    one = pltpu.roll(moments, 128 - 8, 1)
    two = pltpu.roll(moments, 128 - 16, 1)
    squares = two + (2.0 * SHIFT) * one + (SHIFT * SHIFT) * moments
    right = one + SHIFT * moments
    x = [right if h == 0 else pltpu.roll(right, 128 - 8 * h, 1) for h in range(ITERS)]
    tiles = [[lane(squares, 8 * j + v) for v in range(8)] for j in range(2 * ITERS - 1)]
    rows = [[tiles[a + h][i] for h in range(ITERS)] for a in range(ITERS) for i in range(8)]
    size = 8 * ITERS
    for k in range(size):
        g, q = divmod(k, 8)
        column = rows[k]
        inverse = 1.0 / sublane(column[g], q)
        pivot = sublane(x[g], q) * inverse
        for h in range(ITERS):
            x[h] = x[h] - column[h] * pivot
        x[g] = jnp.where(sub == q, pivot, x[g])
        for r in range(k + 1, size):
            factor = sublane(column[r // 8], r % 8) * inverse
            rows[r] = [rows[r][h] - factor * column[h] for h in range(ITERS)]
            rows[r][g] = jnp.where(sub == q, factor, rows[r][g])
    return x


def hessenberg_of(moments):
    sub, lanes = iotas()
    tiles = [[lane(moments, 8 * j + v) for v in range(8)] for j in range(2 * ITERS + 1)]
    groups = ITERS + 1
    rows = [[tiles[a + h][i] for h in range(groups)] for a in range(groups) for i in range(8)]
    size = 8 * groups
    factor_of, scale_of = [], []
    for k in range(size):
        g, q = divmod(k, 8)
        scale = rsqrt(sublane(rows[k][g], q))
        column = [None if h < g else rows[k][h] * scale for h in range(groups)]
        column[g] = jnp.where(sub >= q, column[g], 0.0)
        factor_of.append(column)
        scale_of.append(scale)
        for r in range(k + 1, size):
            factor = sublane(column[r // 8], r % 8)
            for h in range(r // 8, groups):
                rows[r][h] = rows[r][h] - factor * column[h]
    x = []
    for h in range(ITERS):
        tile = jnp.zeros((8, 128), jnp.float32)
        for c in range(8 * (h + 2)):
            tile = jnp.where(lanes == c, factor_of[c][h + 1], tile)
        x.append(tile)
    for k in range(8 * ITERS):
        g, q = divmod(k, 8)
        solved = sublane(x[g], q) * scale_of[k]
        for h in range(g, ITERS):
            x[h] = x[h] - factor_of[k][h] * solved
        x[g] = jnp.where(sub == q, solved, x[g])
    return [x[h] + jnp.where(lanes == 8 * h + sub, SHIFT, 0.0) for h in range(ITERS)]


def kernel(
    n_gz, n_gy, b_ref, d_ref, out_ref, hess_ref,
    field, low_high, side_in, side_out, diag, result, spread, rows_of, moments, gathered,
    load_sem, out_sem, diag_sem, z_send, z_recv, y_send, y_recv, all_send, all_recv,
):
    gz, gy = lax.axis_index("gz"), lax.axis_index("gy")
    n_rows, n_cols = d_ref.shape[1], d_ref.shape[2]
    tiles = n_rows // 8
    core = lax.rem(gz, CORES)
    y_at = lax.rem(lax.div(gz, CORES), Y_CHIPS)
    z_at = lax.div(gz, CORES * Y_CHIPS)
    n_z = n_gz // (CORES * Y_CHIPS)
    own = pl.ds(TOP, n_rows)
    sub, lanes = iotas()

    def load(v):
        return pltpu.make_async_copy(b_ref.at[v], field.at[v, :, own, :], load_sem.at[v])

    diag_copy = pltpu.make_async_copy(d_ref, diag, diag_sem)
    load(0).start()
    load(1).start()
    diag_copy.start()
    for v in range(2, BLK):
        load(v).start()

    def first(i):
        at = lax.rem(gy * CORES + core + i, n_gy * CORES)
        return (gz - core + lax.rem(at, CORES), lax.div(at, CORES))

    def second(i):
        return (gz + (lax.rem(y_at + i, Y_CHIPS) - y_at) * CORES, gy)

    def third(i):
        return (gz + (lax.rem(z_at + i, n_z) - z_at) * CORES * Y_CHIPS, gy)

    stages = (
        (first, n_gy * CORES, gy * CORES + core, 0),
        (second, Y_CHIPS, y_at, n_gy * CORES),
        (third, n_z, z_at, n_gy * CORES + Y_CHIPS),
    )

    barrier = pltpu.get_barrier_semaphore()

    @pl.when(jnp.logical_and(core == 0, gz > 0))
    def _():
        pl.semaphore_signal(barrier, inc=1, device_id=(gz - 1, gy), device_id_type=MESH)

    @pl.when(jnp.logical_and(core == CORES - 1, gz < n_gz - 1))
    def _():
        pl.semaphore_signal(barrier, inc=1, device_id=(gz + 1, gy), device_id_type=MESH)

    count = 0
    for partner, size, _, _ in stages:
        for i in range(1, size):
            pl.semaphore_signal(barrier, inc=1, device_id=partner(i), device_id_type=MESH)
        count += size - 1

    def clear(where, buffer, side):
        @pl.when(where)
        def _():
            @pl.loop(0, ITERS * BLK)
            def _(s):
                buffer[s, side] = jnp.zeros(buffer.shape[2:], jnp.float32)

    clear(gz == 0, low_high, 0)
    clear(gz == n_gz - 1, low_high, 1)
    clear(gy == 0, side_in, 0)
    clear(gy == n_gy - 1, side_in, 1)
    moments[...] = jnp.zeros((8, 128), jnp.float32)

    off_chip = jnp.logical_or(
        jnp.logical_and(core == 0, gz > 0), jnp.logical_and(core == CORES - 1, gz < n_gz - 1)
    )

    pl.semaphore_wait(barrier, count + jnp.where(off_chip, 1, 0))

    def z_copy(s, up):
        return pltpu.make_async_remote_copy(
            src_ref=field.at[s, up, own, :],
            dst_ref=low_high.at[s, 1 - up],
            send_sem=z_send.at[s, up],
            recv_sem=z_recv.at[s, 1 - up],
            device_id=(gz + 2 * up - 1, gy),
            device_id_type=MESH,
        )

    def y_copy(s, up):
        return pltpu.make_async_remote_copy(
            src_ref=side_out.at[s, up],
            dst_ref=side_in.at[s, 1 - up],
            send_sem=y_send.at[s, up],
            recv_sem=y_recv.at[s, 1 - up],
            device_id=(gz, gy + 2 * up - 1),
            device_id_type=MESH,
        )

    has_z = (gz > 0, gz < n_gz - 1)
    has_y = (gy > 0, gy < n_gy - 1)

    def send(s):
        for up in (0, 1):

            @pl.when(has_z[up])
            def _(up=up):
                z_copy(s, up).start()

        for layer in (0, 1):
            side_out[s, 0, layer] = field[s, layer, TOP : TOP + 1, :]
            side_out[s, 1, layer] = field[s, layer, TOP + n_rows - 1 : TOP + n_rows, :]
        for up in (0, 1):

            @pl.when(has_y[up])
            def _(up=up):
                y_copy(s, up).start()

    def arrive(s):
        for up in (0, 1):

            @pl.when(has_z[up])
            def _(up=up):
                z_copy(s, 1 - up).wait_recv()

            @pl.when(has_y[up])
            def _(up=up):
                y_copy(s, 1 - up).wait_recv()

        for layer in (0, 1):
            field[s, layer, TOP - 1 : TOP, :] = side_in[s, 0, layer]
            field[s, layer, TOP + n_rows : TOP + n_rows + 1, :] = side_in[s, 1, layer]

    lane_of_row = lax.broadcasted_iota(jnp.int32, (8, n_cols), 1)

    def apply(s):
        f = s - BLK
        for layer in (0, 1):
            for t in range(tiles):
                low = TOP + 8 * t
                here = field[f, layer, low : low + 8, :]
                beside = field[f, layer, low - 1 : low + 7, :] + field[f, layer, low + 1 : low + 9, :]
                other = field[f, 1 - layer, low : low + 8, :]
                beside = beside + (other + low_high[f, layer, 8 * t : 8 * t + 8, :])
                left = jnp.where(lane_of_row == 0, 0.0, pltpu.roll(here, 1, 1))
                right = jnp.where(lane_of_row == n_cols - 1, 0.0, pltpu.roll(here, n_cols - 1, 1))
                field[s, layer, low : low + 8, :] = diag[layer, 8 * t : 8 * t + 8, :] * here - (
                    beside + (left + right)
                )

    def fold(row):
        total = row[:, :128]
        for at in range(128, n_cols, 128):
            total = total + row[:, at : at + 128]
        return jnp.sum(total, axis=0, keepdims=True)

    def products(s, v, others):
        @pl.loop(0, v + 1)
        def _(u):
            totals = [jnp.zeros((8, n_cols), jnp.float32) for _ in others]
            for layer in (0, 1):
                for t in range(tiles):
                    low = TOP + 8 * t
                    here = field[s, layer, low : low + 8, :]
                    totals = [
                        total + here * field[u + other, layer, low : low + 8, :]
                        for total, other in zip(totals, others)
                    ]
            for at, total in enumerate(totals):
                rows_of[at, pl.ds(u, 1), :] = fold(total)

    def place(at, j, v):
        values = jnp.sum(rows_of[at], axis=1, keepdims=True)
        values = jnp.where(sub <= v, values, 0.0)
        new = jnp.where(lanes == j * 8 + v, values, 0.0)
        turned = jnp.where(jnp.logical_and(lanes == j * 8 + sub, sub < v), values, 0.0)
        turned = jnp.sum(turned, axis=0, keepdims=True)
        moments[...] = moments[...] + (new + jnp.where(sub == v, turned, 0.0))

    rows_of[...] = jnp.zeros(rows_of.shape, jnp.float32)

    @pl.loop(0, BLK)
    def _(v):
        load(v).wait()
        send(v)
        products(v, v, (0,))
        place(0, 0, v)

    diag_copy.wait()
    diag[...] = diag[...] + (6.0 - SHIFT)

    @pl.loop(BLK, (ITERS + 1) * BLK)
    def _(s):
        k, v = lax.div(s, BLK), lax.rem(s, BLK)
        arrive(s - BLK)
        apply(s)

        @pl.when(s < ITERS * BLK)
        def _():
            send(s)

        products(s, v, (k * BLK - BLK, k * BLK))
        place(0, 2 * k - 1, v)
        place(1, 2 * k, v)

    total = moments[...]
    for at, (partner, size, me, base) in enumerate(stages):
        gathered[base + me] = total

        def copy(i):
            return pltpu.make_async_remote_copy(
                src_ref=gathered.at[base + me],
                dst_ref=gathered.at[base + me],
                send_sem=all_send.at[base + i],
                recv_sem=all_recv.at[base + i],
                device_id=partner(i),
                device_id_type=MESH,
            )

        for i in range(1, size):
            copy(i).start()
        for i in range(1, size):
            copy(i).wait_recv()
        total = gathered[base]
        for i in range(1, size):
            total = total + gathered[base + i]
        for i in range(1, size):
            copy(i).wait_send()

    weights = weights_of(total)
    for h in range(ITERS):
        for i in range(BLK):
            spread[i, 8 * h : 8 * h + 8, :] = lane(weights[h], i)
    for h, tile in enumerate(hessenberg_of(total)):
        hess_ref[8 * h : 8 * h + 8, :] = tile[:, : hess_ref.shape[1]]

    def store(i):
        return pltpu.make_async_copy(result.at[i], out_ref.at[i], out_sem.at[i])

    @pl.loop(0, BLK)
    def _(i):
        factors = [
            jnp.broadcast_to(spread[i, j : j + 1, :], (8, 128)) for j in range(ITERS * BLK)
        ]
        for layer in (0, 1):

            @pl.loop(0, tiles)
            def _(t):
                low = pl.multiple_of(8 * t, 8)
                for at in range(0, n_cols, 128):
                    parts = [None] * 4
                    for j in range(ITERS * BLK):
                        term = factors[j] * field[j, layer, pl.ds(TOP + low, 8), at : at + 128]
                        parts[j % 4] = term if parts[j % 4] is None else parts[j % 4] + term
                    result[i, layer, pl.ds(low, 8), at : at + 128] = (parts[0] + parts[1]) + (
                        parts[2] + parts[3]
                    )

        store(i).start()

    @pl.loop(0, ITERS * BLK)
    def _(s):
        for up in (0, 1):

            @pl.when(has_z[up])
            def _(up=up):
                z_copy(s, up).wait_send()

            @pl.when(has_y[up])
            def _(up=up):
                y_copy(s, up).wait_send()

    @pl.loop(0, BLK)
    def _(i):
        store(i).wait()


def solution(mesh):
    n_gz, n_gy = mesh.shape["gz"], mesh.shape["gy"]
    n_z = n_gz // (CORES * Y_CHIPS)
    partners = n_gy * CORES + Y_CHIPS + n_z

    def body(right_side, diagonal):
        layers, n_rows, n_cols = diagonal.shape
        powers = ITERS * BLK
        vmem = lambda *shape: pltpu.VMEM(shape, jnp.float32)
        dma = pltpu.SemaphoreType.DMA
        return pl.pallas_call(
            functools.partial(kernel, n_gz, n_gy),
            out_shape=(
                jax.ShapeDtypeStruct(right_side.shape, jnp.float32),
                jax.ShapeDtypeStruct((powers, powers + BLK), jnp.float32),
            ),
            in_specs=[pl.BlockSpec(memory_space=pltpu.HBM)] * 2,
            out_specs=(
                pl.BlockSpec(memory_space=pltpu.HBM),
                pl.BlockSpec(memory_space=pltpu.VMEM),
            ),
            scratch_shapes=[
                vmem(powers + BLK, layers, n_rows + 2 * TOP, n_cols),
                vmem(powers, 2, n_rows, n_cols),
                vmem(powers, 2, layers, 1, n_cols),
                vmem(powers, 2, layers, 1, n_cols),
                vmem(layers, n_rows, n_cols),
                vmem(BLK, layers, n_rows, n_cols),
                vmem(BLK, powers, 128),
                vmem(2, 8, 128),
                vmem(8, 128),
                vmem(partners, 8, 128),
                dma((BLK,)),
                dma((BLK,)),
                dma,
                dma((powers, 2)),
                dma((powers, 2)),
                dma((powers, 2)),
                dma((powers, 2)),
                dma((partners,)),
                dma((partners,)),
            ],
            compiler_params=pltpu.CompilerParams(collective_id=0, has_side_effects=True),
            name="block_gmres",
        )(right_side, diagonal)

    placed = (P(None, "gz", "gy", None), P("gz", "gy", None))
    return jax.shard_map(
        body, mesh=mesh, in_specs=placed, out_specs=(placed[0], P()), check_vma=False
    )
```

```python
import functools

import jax
import jax.numpy as jnp
from jax import lax
from jax.experimental import pallas as pl
from jax.experimental.pallas import tpu as pltpu
from jax.sharding import PartitionSpec as P

MESH = pl.DeviceIdType.MESH
BLK = 8
ITERS = 3
SHIFT = 7.0
TOP = 8
Y_CHIPS = 4
CORES = 2


def iotas():
    return (
        lax.broadcasted_iota(jnp.int32, (8, 128), 0),
        lax.broadcasted_iota(jnp.int32, (8, 128), 1),
    )


def sublane(tile, at):
    return jnp.broadcast_to(tile[at : at + 1, :], (8, 128))


def lane(tile, at):
    return jnp.broadcast_to(tile[:, at : at + 1], (8, 128))


def rsqrt(value):
    guess = lax.rsqrt(value)
    return guess * (1.5 - 0.5 * value * guess * guess)


def weights_of(moments):
    sub, _ = iotas()
    one = pltpu.roll(moments, 128 - 8, 1)
    two = pltpu.roll(moments, 128 - 16, 1)
    squares = two + (2.0 * SHIFT) * one + (SHIFT * SHIFT) * moments
    right = one + SHIFT * moments
    x = [right if h == 0 else pltpu.roll(right, 128 - 8 * h, 1) for h in range(ITERS)]
    tiles = [[lane(squares, 8 * j + v) for v in range(8)] for j in range(2 * ITERS - 1)]
    rows = [[tiles[a + h][i] for h in range(ITERS)] for a in range(ITERS) for i in range(8)]
    size = 8 * ITERS
    for k in range(size):
        g, q = divmod(k, 8)
        column = rows[k]
        inverse = 1.0 / sublane(column[g], q)
        pivot = sublane(x[g], q) * inverse
        for h in range(ITERS):
            x[h] = x[h] - column[h] * pivot
        x[g] = jnp.where(sub == q, pivot, x[g])
        for r in range(k + 1, size):
            factor = sublane(column[r // 8], r % 8) * inverse
            rows[r] = [rows[r][h] - factor * column[h] for h in range(ITERS)]
            rows[r][g] = jnp.where(sub == q, factor, rows[r][g])
    return x


def hessenberg_of(moments):
    sub, lanes = iotas()
    tiles = [[lane(moments, 8 * j + v) for v in range(8)] for j in range(2 * ITERS + 1)]
    groups = ITERS + 1
    rows = [[tiles[a + h][i] for h in range(groups)] for a in range(groups) for i in range(8)]
    size = 8 * groups
    factor_of, scale_of = [], []
    for k in range(size):
        g, q = divmod(k, 8)
        scale = rsqrt(sublane(rows[k][g], q))
        column = [None if h < g else rows[k][h] * scale for h in range(groups)]
        column[g] = jnp.where(sub >= q, column[g], 0.0)
        factor_of.append(column)
        scale_of.append(scale)
        for r in range(k + 1, size):
            factor = sublane(column[r // 8], r % 8)
            for h in range(r // 8, groups):
                rows[r][h] = rows[r][h] - factor * column[h]
    x = []
    for h in range(ITERS):
        tile = jnp.zeros((8, 128), jnp.float32)
        for c in range(8 * (h + 2)):
            tile = jnp.where(lanes == c, factor_of[c][h + 1], tile)
        x.append(tile)
    for k in range(8 * ITERS):
        g, q = divmod(k, 8)
        solved = sublane(x[g], q) * scale_of[k]
        for h in range(g, ITERS):
            x[h] = x[h] - factor_of[k][h] * solved
        x[g] = jnp.where(sub == q, solved, x[g])
    return [x[h] + jnp.where(lanes == 8 * h + sub, SHIFT, 0.0) for h in range(ITERS)]


def kernel(
    n_gz, n_gy, b_ref, d_ref, high_ref, low_ref, mix_ref, hess_ref,
    field, low_high, side_in, side_out, diag, rows_of, moments, gathered,
    load_sem, diag_sem, z_send, z_recv, y_send, y_recv, all_send, all_recv, ready,
):
    gz, gy = lax.axis_index("gz"), lax.axis_index("gy")
    n_rows, n_cols = d_ref.shape[1], d_ref.shape[2]
    tiles = n_rows // 8
    core = lax.rem(gz, CORES)
    y_at = lax.rem(lax.div(gz, CORES), Y_CHIPS)
    z_at = lax.div(gz, CORES * Y_CHIPS)
    n_z = n_gz // (CORES * Y_CHIPS)
    own = pl.ds(TOP, n_rows)
    sub, lanes = iotas()

    def load(v):
        return pltpu.make_async_copy(b_ref.at[v], field.at[v, :, own, :], load_sem.at[v])

    diag_copy = pltpu.make_async_copy(d_ref, diag, diag_sem)
    load(0).start()
    load(1).start()
    diag_copy.start()
    for v in range(2, BLK):
        load(v).start()

    def x_core(i):
        at = lax.rem(gy * CORES + core + i, n_gy * CORES)
        return (gz - core + lax.rem(at, CORES), lax.div(at, CORES))

    def along_y(i):
        return (gz + (lax.rem(y_at + i, Y_CHIPS) - y_at) * CORES, gy)

    def along_z(i):
        return (gz + (lax.rem(z_at + i, n_z) - z_at) * CORES * Y_CHIPS, gy)

    def first(i):
        at = lax.rem(y_at * n_gy + gy + i, Y_CHIPS * n_gy)
        return (gz + (lax.div(at, n_gy) - y_at) * CORES, lax.rem(at, n_gy))

    def second(i):
        at = lax.rem(z_at * CORES + core + i, n_z * CORES)
        return (
            gz + (lax.div(at, CORES) - z_at) * CORES * Y_CHIPS + lax.rem(at, CORES) - core,
            gy,
        )

    stages = (
        (first, Y_CHIPS * n_gy, y_at * n_gy + gy, 0),
        (second, n_z * CORES, z_at * CORES + core, Y_CHIPS * n_gy),
    )

    barrier = pltpu.get_barrier_semaphore()

    @pl.when(jnp.logical_and(core == 0, gz > 0))
    def _():
        pl.semaphore_signal(barrier, inc=1, device_id=(gz - 1, gy), device_id_type=MESH)

    @pl.when(jnp.logical_and(core == CORES - 1, gz < n_gz - 1))
    def _():
        pl.semaphore_signal(barrier, inc=1, device_id=(gz + 1, gy), device_id_type=MESH)

    count = 0
    for partner, size in ((along_z, n_z), (along_y, Y_CHIPS), (x_core, n_gy * CORES)):
        for i in range(1, size):
            pl.semaphore_signal(barrier, inc=1, device_id=partner(i), device_id_type=MESH)
        count += size - 1

    def clear(where, buffer, side):
        @pl.when(where)
        def _():
            @pl.loop(0, ITERS * BLK)
            def _(s):
                buffer[s, side] = jnp.zeros(buffer.shape[2:], jnp.float32)

    clear(gz == 0, low_high, 0)
    clear(gz == n_gz - 1, low_high, 1)
    clear(gy == 0, side_in, 0)
    clear(gy == n_gy - 1, side_in, 1)
    moments[...] = jnp.zeros((8, 128), jnp.float32)

    off_chip = jnp.logical_or(
        jnp.logical_and(core == 0, gz > 0), jnp.logical_and(core == CORES - 1, gz < n_gz - 1)
    )

    pl.semaphore_wait(barrier, count + jnp.where(off_chip, 1, 0))

    def z_copy(s, up):
        return pltpu.make_async_remote_copy(
            src_ref=field.at[s, up, own, :],
            dst_ref=low_high.at[s, 1 - up],
            send_sem=z_send.at[s, up],
            recv_sem=z_recv.at[s, 1 - up],
            device_id=(gz + 2 * up - 1, gy),
            device_id_type=MESH,
        )

    def y_copy(s, up):
        return pltpu.make_async_remote_copy(
            src_ref=side_out.at[s, up],
            dst_ref=side_in.at[s, 1 - up],
            send_sem=y_send.at[s, up],
            recv_sem=y_recv.at[s, 1 - up],
            device_id=(gz, gy + 2 * up - 1),
            device_id_type=MESH,
        )

    has_z = (gz > 0, gz < n_gz - 1)
    has_y = (gy > 0, gy < n_gy - 1)

    def send(s):
        for up in (0, 1):

            @pl.when(has_z[up])
            def _(up=up):
                z_copy(s, up).start()

        for layer in (0, 1):
            side_out[s, 0, layer] = field[s, layer, TOP : TOP + 1, :]
            side_out[s, 1, layer] = field[s, layer, TOP + n_rows - 1 : TOP + n_rows, :]
        for up in (0, 1):

            @pl.when(has_y[up])
            def _(up=up):
                y_copy(s, up).start()

    def arrive(s):
        for up in (0, 1):

            @pl.when(has_z[up])
            def _(up=up):
                z_copy(s, 1 - up).wait_recv()

            @pl.when(has_y[up])
            def _(up=up):
                y_copy(s, 1 - up).wait_recv()

        for layer in (0, 1):
            field[s, layer, TOP - 1 : TOP, :] = side_in[s, 0, layer]
            field[s, layer, TOP + n_rows : TOP + n_rows + 1, :] = side_in[s, 1, layer]

    lane_of_row = lax.broadcasted_iota(jnp.int32, (8, n_cols), 1)

    def apply(s):
        f = s - BLK
        for layer in (0, 1):
            for t in range(tiles):
                low = TOP + 8 * t
                here = field[f, layer, low : low + 8, :]
                beside = field[f, layer, low - 1 : low + 7, :] + field[f, layer, low + 1 : low + 9, :]
                other = field[f, 1 - layer, low : low + 8, :]
                beside = beside + (other + low_high[f, layer, 8 * t : 8 * t + 8, :])
                left = jnp.where(lane_of_row == 0, 0.0, pltpu.roll(here, 1, 1))
                right = jnp.where(lane_of_row == n_cols - 1, 0.0, pltpu.roll(here, n_cols - 1, 1))
                field[s, layer, low : low + 8, :] = diag[layer, 8 * t : 8 * t + 8, :] * here - (
                    beside + (left + right)
                )

    def fold(row):
        total = row[:, :128]
        for at in range(128, n_cols, 128):
            total = total + row[:, at : at + 128]
        return jnp.sum(total, axis=0, keepdims=True)

    def products(s, v, others):
        @pl.loop(0, v + 1)
        def _(u):
            totals = [jnp.zeros((8, n_cols), jnp.float32) for _ in others]
            for layer in (0, 1):
                for t in range(tiles):
                    low = TOP + 8 * t
                    here = field[s, layer, low : low + 8, :]
                    totals = [
                        total + here * field[u + other, layer, low : low + 8, :]
                        for total, other in zip(totals, others)
                    ]
            for at, total in enumerate(totals):
                rows_of[at, pl.ds(u, 1), :] = fold(total)

    def place(at, j, v):
        values = jnp.sum(rows_of[at], axis=1, keepdims=True)
        values = jnp.where(sub <= v, values, 0.0)
        new = jnp.where(lanes == j * 8 + v, values, 0.0)
        turned = jnp.where(jnp.logical_and(lanes == j * 8 + sub, sub < v), values, 0.0)
        turned = jnp.sum(turned, axis=0, keepdims=True)
        moments[...] = moments[...] + (new + jnp.where(sub == v, turned, 0.0))

    def split(k, part):
        for layer in (0, 1):
            low = pl.multiple_of(TOP + 8 * part, 8)
            values = field[pl.ds(k * BLK, BLK), layer, pl.ds(low, 8), :].reshape(8 * BLK, n_cols)
            high = values.astype(jnp.bfloat16)
            to = pl.ds(pl.multiple_of(k * (8 * BLK), 8 * BLK), 8 * BLK)
            high_ref[layer * tiles + part, to, :] = high
            low_ref[layer * tiles + part, to, :] = (values - high.astype(jnp.float32)).astype(
                jnp.bfloat16
            )

    rows_of[...] = jnp.zeros(rows_of.shape, jnp.float32)

    @pl.loop(0, BLK)
    def _(v):
        load(v).wait()
        send(v)

    for partner, size in ((along_z, n_z), (along_y, Y_CHIPS)):
        for i in range(1, size):
            pl.semaphore_signal(ready, inc=1, device_id=partner(i), device_id_type=MESH)

    @pl.loop(0, BLK)
    def _(v):
        products(v, v, (0,))
        place(0, 0, v)

    diag_copy.wait()
    diag[...] = diag[...] + (6.0 - SHIFT)

    @pl.loop(BLK, (ITERS + 1) * BLK)
    def _(s):
        k, v = lax.div(s, BLK), lax.rem(s, BLK)
        arrive(s - BLK)
        apply(s)

        @pl.when(s < ITERS * BLK)
        def _():
            send(s)

        products(s, v, (k * BLK - BLK, k * BLK))
        place(0, 2 * k - 1, v)
        place(1, 2 * k, v)

        split(k - 1, v)

    pl.semaphore_wait(ready, (n_z - 1) + (Y_CHIPS - 1))

    def copy(stage, i):
        partner, _, me, base = stage
        return pltpu.make_async_remote_copy(
            src_ref=gathered.at[base + me],
            dst_ref=gathered.at[base + me],
            send_sem=all_send.at[base + i],
            recv_sem=all_recv.at[base + i],
            device_id=partner(i),
            device_id_type=MESH,
        )

    total = moments[...]
    for stage in stages:
        _, size, me, base = stage
        gathered[base + me] = total
        for i in range(1, size):
            copy(stage, i).start()
        for i in range(1, size):
            copy(stage, i).wait_recv()
        total = gathered[base]
        for i in range(1, size):
            total = total + gathered[base + i]

    weights = weights_of(total)
    eighth, within = lax.div(lanes, 8), lax.rem(lanes, 8)
    for i in range(0, BLK, 2):
        wide = []
        for at in (i, i + 1):
            column = [lane(weights[h], at) for h in range(ITERS)]
            front = jnp.where(eighth == sub, column[0], 0.0) + jnp.where(
                eighth == sub + 8, column[1], 0.0
            )
            back = jnp.where(eighth == sub, column[2], 0.0)
            wide.append(
                [
                    jnp.where(within == sub, jnp.sum(part, axis=0, keepdims=True), 0.0)
                    for part in (front, back)
                ]
            )
        for part, (start, stop) in enumerate(((0, 128), (128, 8 * BLK * ITERS))):
            both = jnp.concatenate([wide[0][part], wide[1][part]], axis=0)
            high = both.astype(jnp.bfloat16)
            low = (both - high.astype(jnp.float32)).astype(jnp.bfloat16)
            mix_ref[8 * i : 8 * i + 16, start:stop] = high[:, : stop - start]
            mix_ref[64 + 8 * i : 64 + 8 * i + 16, start:stop] = low[:, : stop - start]
    for h, tile in enumerate(hessenberg_of(total)):
        hess_ref[8 * h : 8 * h + 8, :] = tile[:, : hess_ref.shape[1]]

    @pl.loop(0, ITERS * BLK)
    def _(s):
        for up in (0, 1):

            @pl.when(has_z[up])
            def _(up=up):
                z_copy(s, up).wait_send()

            @pl.when(has_y[up])
            def _(up=up):
                y_copy(s, up).wait_send()

    for stage in stages:
        for i in range(1, stage[1]):
            copy(stage, i).wait_send()


def combine(high_ref, low_ref, mix_ref, h_ref, out_ref, hess_ref, result, out_sem):
    hess_ref[...] = h_ref[...]
    tiles = high_ref.shape[0] // 2

    def store(n):
        where = (slice(None), n // tiles, pl.ds(8 * (n % tiles), 8))
        return pltpu.make_async_copy(result.at[where], out_ref.at[where], out_sem.at[n])

    for n in range(2 * tiles):
        both = jnp.dot(mix_ref[...], high_ref[n], preferred_element_type=jnp.float32)
        rest = jnp.dot(mix_ref[:64], low_ref[n], preferred_element_type=jnp.float32)
        total = both[:64] + (both[64:] + rest)
        result[:, n // tiles, 8 * (n % tiles) : 8 * (n % tiles) + 8, :] = total.reshape(
            BLK, 8, total.shape[1]
        )
        store(n).start()
    for n in range(2 * tiles):
        store(n).wait()


def solution(mesh):
    n_gz, n_gy = mesh.shape["gz"], mesh.shape["gy"]
    n_z = n_gz // (CORES * Y_CHIPS)
    partners = n_gy * Y_CHIPS + n_z * CORES

    def body(right_side, diagonal):
        layers, n_rows, n_cols = diagonal.shape
        powers = ITERS * BLK
        pieces = layers * n_rows // 8
        vmem = lambda *shape: pltpu.VMEM(shape, jnp.float32)
        dma = pltpu.SemaphoreType.DMA
        whole = pl.BlockSpec(memory_space=pltpu.VMEM)
        high, low, mix, hessenberg = pl.pallas_call(
            functools.partial(kernel, n_gz, n_gy),
            out_shape=(
                jax.ShapeDtypeStruct((pieces, 8 * powers, n_cols), jnp.bfloat16),
                jax.ShapeDtypeStruct((pieces, 8 * powers, n_cols), jnp.bfloat16),
                jax.ShapeDtypeStruct((16 * BLK, 8 * powers), jnp.bfloat16),
                jax.ShapeDtypeStruct((powers, powers + BLK), jnp.float32),
            ),
            in_specs=[pl.BlockSpec(memory_space=pltpu.HBM)] * 2,
            out_specs=(whole,) * 4,
            scratch_shapes=[
                vmem(powers + BLK, layers, n_rows + 2 * TOP, n_cols),
                vmem(powers, 2, n_rows, n_cols),
                vmem(powers, 2, layers, 1, n_cols),
                vmem(powers, 2, layers, 1, n_cols),
                vmem(layers, n_rows, n_cols),
                vmem(2, 8, 128),
                vmem(8, 128),
                vmem(partners, 8, 128),
                dma((BLK,)),
                dma,
                dma((powers, 2)),
                dma((powers, 2)),
                dma((powers, 2)),
                dma((powers, 2)),
                dma((partners,)),
                dma((partners,)),
                pltpu.SemaphoreType.REGULAR,
            ],
            compiler_params=pltpu.CompilerParams(
                collective_id=0, has_side_effects=True, vmem_limit_bytes=28 << 20
            ),
            name="block_gmres",
        )(*(pltpu.with_memory_space_constraint(a, pltpu.HBM) for a in (right_side, diagonal)))
        return pl.pallas_call(
            combine,
            out_shape=(
                jax.ShapeDtypeStruct(right_side.shape, jnp.float32),
                jax.ShapeDtypeStruct(hessenberg.shape, jnp.float32),
            ),
            in_specs=[whole] * 4,
            out_specs=(pl.BlockSpec(memory_space=pltpu.HBM), whole),
            scratch_shapes=[vmem(*right_side.shape), dma((pieces,))],
            compiler_params=pltpu.CompilerParams(vmem_limit_bytes=12 << 20),
            name="combine",
        )(high, low, mix, hessenberg)

    placed = (P(None, "gz", "gy", None), P("gz", "gy", None))
    return jax.shard_map(
        body, mesh=mesh, in_specs=placed, out_specs=(placed[0], P()), check_vma=False
    )
```

```python
import functools

import jax
import jax.numpy as jnp
from jax import lax
from jax.experimental import pallas as pl
from jax.experimental.pallas import tpu as pltpu
from jax.sharding import PartitionSpec as P

MESH = pl.DeviceIdType.MESH
BLK = 8
ITERS = 3
SHIFT = 7.0
TOP = 8
Y_CHIPS = 4
CORES = 2


def iotas():
    return (
        lax.broadcasted_iota(jnp.int32, (8, 128), 0),
        lax.broadcasted_iota(jnp.int32, (8, 128), 1),
    )


def sublane(tile, at):
    return jnp.broadcast_to(tile[at : at + 1, :], (8, 128))


def lane(tile, at):
    return jnp.broadcast_to(tile[:, at : at + 1], (8, 128))


def rsqrt(value):
    guess = lax.rsqrt(value)
    return guess * (1.5 - 0.5 * value * guess * guess)


def weights_of(moments):
    sub, _ = iotas()
    one = pltpu.roll(moments, 128 - 8, 1)
    two = pltpu.roll(moments, 128 - 16, 1)
    squares = two + (2.0 * SHIFT) * one + (SHIFT * SHIFT) * moments
    right = one + SHIFT * moments
    x = [right if h == 0 else pltpu.roll(right, 128 - 8 * h, 1) for h in range(ITERS)]
    tiles = [[lane(squares, 8 * j + v) for v in range(8)] for j in range(2 * ITERS - 1)]
    rows = [[tiles[a + h][i] for h in range(ITERS)] for a in range(ITERS) for i in range(8)]
    size = 8 * ITERS
    for k in range(size):
        g, q = divmod(k, 8)
        column = rows[k]
        inverse = 1.0 / sublane(column[g], q)
        pivot = sublane(x[g], q) * inverse
        for h in range(ITERS):
            x[h] = x[h] - column[h] * pivot
        x[g] = jnp.where(sub == q, pivot, x[g])
        for r in range(k + 1, size):
            factor = sublane(column[r // 8], r % 8) * inverse
            rows[r] = [rows[r][h] - factor * column[h] for h in range(ITERS)]
            rows[r][g] = jnp.where(sub == q, factor, rows[r][g])
    return x


def hessenberg_of(moments):
    sub, lanes = iotas()
    tiles = [[lane(moments, 8 * j + v) for v in range(8)] for j in range(2 * ITERS + 1)]
    groups = ITERS + 1
    rows = [[tiles[a + h][i] for h in range(groups)] for a in range(groups) for i in range(8)]
    size = 8 * groups
    factor_of, scale_of = [], []
    for k in range(size):
        g, q = divmod(k, 8)
        scale = rsqrt(sublane(rows[k][g], q))
        column = [None if h < g else rows[k][h] * scale for h in range(groups)]
        column[g] = jnp.where(sub >= q, column[g], 0.0)
        factor_of.append(column)
        scale_of.append(scale)
        for r in range(k + 1, size):
            factor = sublane(column[r // 8], r % 8)
            for h in range(r // 8, groups):
                rows[r][h] = rows[r][h] - factor * column[h]
    x = []
    for h in range(ITERS):
        tile = jnp.zeros((8, 128), jnp.float32)
        for c in range(8 * (h + 2)):
            tile = jnp.where(lanes == c, factor_of[c][h + 1], tile)
        x.append(tile)
    for k in range(8 * ITERS):
        g, q = divmod(k, 8)
        solved = sublane(x[g], q) * scale_of[k]
        for h in range(g, ITERS):
            x[h] = x[h] - factor_of[k][h] * solved
        x[g] = jnp.where(sub == q, solved, x[g])
    return [x[h] + jnp.where(lanes == 8 * h + sub, SHIFT, 0.0) for h in range(ITERS)]


def kernel(
    n_gz, n_gy, b_ref, d_ref, high_ref, low_ref, mix_ref, sum_ref,
    field, low_high, side_in, side_out, diag, rows_of, moments, gathered,
    load_sem, diag_sem, z_send, z_recv, y_send, y_recv, all_send, all_recv, ready,
):
    gz, gy = lax.axis_index("gz"), lax.axis_index("gy")
    n_rows, n_cols = d_ref.shape[1], d_ref.shape[2]
    tiles = n_rows // 8
    core = lax.rem(gz, CORES)
    y_at = lax.rem(lax.div(gz, CORES), Y_CHIPS)
    z_at = lax.div(gz, CORES * Y_CHIPS)
    n_z = n_gz // (CORES * Y_CHIPS)
    fast = 1 - core
    own = pl.ds(TOP, n_rows)
    sub, lanes = iotas()

    def load(v):
        return pltpu.make_async_copy(b_ref.at[v], field.at[v, :, own, :], load_sem.at[v])

    diag_copy = pltpu.make_async_copy(d_ref, diag, diag_sem)
    load(0).start()
    load(1).start()
    diag_copy.start()
    for v in range(2, BLK):
        load(v).start()

    def around(at, i, size):
        return at + i if i == 0 else jnp.where(at + i >= size, at + (i - size), at + i)

    def first(i):
        return (gz + (around(y_at, i // n_gy, Y_CHIPS) - y_at) * CORES, around(gy, i % n_gy, n_gy))

    def second(i):
        to = (around(z_at, i // CORES, n_z) - z_at) * CORES * Y_CHIPS
        return (gz + to + around(core, i % CORES, CORES) - core, gy)

    stages = (
        (first, Y_CHIPS * n_gy, y_at * n_gy + gy, 0),
        (second, n_z * CORES, z_at * CORES + core, Y_CHIPS * n_gy),
    )

    def tell(semaphore, gz_step, gy_step):
        count = 0
        for sign in (-1, 1):
            to_gz, to_gy = gz + sign * gz_step, gy + sign * gy_step
            there = jnp.logical_and(
                jnp.logical_and(to_gz >= 0, to_gz < n_gz), jnp.logical_and(to_gy >= 0, to_gy < n_gy)
            )

            @pl.when(there)
            def _(to_gz=to_gz, to_gy=to_gy):
                pl.semaphore_signal(
                    semaphore, inc=1, device_id=(to_gz, to_gy), device_id_type=MESH
                )

            count += jnp.where(there, 1, 0)
        return count

    barrier = pltpu.get_barrier_semaphore()
    expected = tell(barrier, 1, 0) + tell(barrier, 0, 1)

    def clear(where, buffer, side):
        @pl.when(where)
        def _():
            @pl.loop(0, ITERS * BLK)
            def _(s):
                buffer[s, side] = jnp.zeros(buffer.shape[2:], jnp.float32)

    clear(gz == 0, low_high, 0)
    clear(gz == n_gz - 1, low_high, 1)
    clear(gy == 0, side_in, 0)
    clear(gy == n_gy - 1, side_in, 1)
    moments[...] = jnp.zeros((8, 128), jnp.float32)

    off_chip = jnp.where(core == 0, gz > 0, gz < n_gz - 1)

    pl.semaphore_wait(barrier, expected)

    rounds = []
    step = 1
    while step < n_gz:
        rounds.append((step, 0))
        step *= 2
    rounds += [(0, 1)] * (n_gy - 1)

    def knows(r):
        gz_step, gy_step = rounds[r]
        count = 0
        for sign in (-1, 1):
            to_gz, to_gy = gz + sign * gz_step, gy + sign * gy_step
            there = jnp.logical_and(
                jnp.logical_and(to_gz >= 0, to_gz < n_gz), jnp.logical_and(to_gy >= 0, to_gy < n_gy)
            )
            count += jnp.where(there, 1, 0)
        pl.semaphore_wait(ready.at[r], count)

    def z_copy(s, up):
        return pltpu.make_async_remote_copy(
            src_ref=field.at[s, up, own, :],
            dst_ref=low_high.at[s, 1 - up],
            send_sem=z_send.at[s, up],
            recv_sem=z_recv.at[s, 1 - up],
            device_id=(gz + 2 * up - 1, gy),
            device_id_type=MESH,
        )

    def y_copy(s, up):
        return pltpu.make_async_remote_copy(
            src_ref=side_out.at[s, up],
            dst_ref=side_in.at[s, 1 - up],
            send_sem=y_send.at[s, up],
            recv_sem=y_recv.at[s, 1 - up],
            device_id=(gz, gy + 2 * up - 1),
            device_id_type=MESH,
        )

    has_y = (gy > 0, gy < n_gy - 1)

    def send_z(s, layer):
        if layer is fast:
            z_copy(s, fast).start()
        else:

            @pl.when(off_chip)
            def _():
                z_copy(s, core).start()

    def send_y(s):
        for layer in (0, 1):
            side_out[s, 0, layer] = field[s, layer, TOP : TOP + 1, :]
            side_out[s, 1, layer] = field[s, layer, TOP + n_rows - 1 : TOP + n_rows, :]
        for up in (0, 1):

            @pl.when(has_y[up])
            def _(up=up):
                y_copy(s, up).start()

    def arrive_y(s):
        for up in (0, 1):

            @pl.when(has_y[up])
            def _(up=up):
                y_copy(s, 1 - up).wait_recv()

        for layer in (0, 1):
            field[s, layer, TOP - 1 : TOP, :] = side_in[s, 0, layer]
            field[s, layer, TOP + n_rows : TOP + n_rows + 1, :] = side_in[s, 1, layer]

    def arrive_z(s, layer):
        if layer is fast:
            z_copy(s, core).wait_recv()
        else:

            @pl.when(off_chip)
            def _():
                z_copy(s, fast).wait_recv()

    lane_of_row = lax.broadcasted_iota(jnp.int32, (8, n_cols), 1)

    def apply(s, layer):
        f = s - BLK
        for t in range(tiles):
            low = TOP + 8 * t
            here = field[f, layer, low : low + 8, :]
            beside = field[f, layer, low - 1 : low + 7, :] + field[f, layer, low + 1 : low + 9, :]
            other = field[f, 1 - layer, low : low + 8, :]
            beside = beside + (other + low_high[f, layer, 8 * t : 8 * t + 8, :])
            left = jnp.where(lane_of_row == 0, 0.0, pltpu.roll(here, 1, 1))
            right = jnp.where(lane_of_row == n_cols - 1, 0.0, pltpu.roll(here, n_cols - 1, 1))
            field[s, layer, low : low + 8, :] = diag[layer, 8 * t : 8 * t + 8, :] * here - (
                beside + (left + right)
            )

    def fold(row):
        total = row[:, :128]
        for at in range(128, n_cols, 128):
            total = total + row[:, at : at + 128]
        return jnp.sum(total, axis=0, keepdims=True)

    def products(s, v, others, layers, more=False):
        @pl.loop(0, v + 1)
        def _(u):
            totals = [jnp.zeros((8, n_cols), jnp.float32) for _ in others]
            for layer in layers:
                for t in range(tiles):
                    low = TOP + 8 * t
                    here = field[s, layer, low : low + 8, :]
                    totals = [
                        total + here * field[u + other, layer, low : low + 8, :]
                        for total, other in zip(totals, others)
                    ]
            for at, total in enumerate(totals):
                new = fold(total)
                if more:
                    new = new + rows_of[at, pl.ds(u, 1), :]
                rows_of[at, pl.ds(u, 1), :] = new

    def place(at, j, v):
        values = jnp.sum(rows_of[at], axis=1, keepdims=True)
        values = jnp.where(sub <= v, values, 0.0)
        new = jnp.where(lanes == j * 8 + v, values, 0.0)
        turned = jnp.where(jnp.logical_and(lanes == j * 8 + sub, sub < v), values, 0.0)
        turned = jnp.sum(turned, axis=0, keepdims=True)
        moments[...] = moments[...] + (new + jnp.where(sub == v, turned, 0.0))

    def split(k, part):
        for layer in (0, 1):
            low = pl.multiple_of(TOP + 8 * part, 8)
            values = field[pl.ds(k * BLK, BLK), layer, pl.ds(low, 8), :].reshape(8 * BLK, n_cols)
            high = values.astype(jnp.bfloat16)
            to = pl.ds(pl.multiple_of(k * (8 * BLK), 8 * BLK), 8 * BLK)
            high_ref[layer * tiles + part, to, :] = high
            low_ref[layer * tiles + part, to, :] = (values - high.astype(jnp.float32)).astype(
                jnp.bfloat16
            )

    rows_of[...] = jnp.zeros(rows_of.shape, jnp.float32)

    @pl.loop(0, BLK)
    def _(v):
        load(v).wait()
        send_z(v, core)
        send_z(v, fast)
        send_y(v)

    @pl.loop(0, BLK)
    def _(v):
        products(v, v, (0,), (0, 1))
        place(0, 0, v)

    diag_copy.wait()
    diag[...] = diag[...] + (6.0 - SHIFT)

    @pl.loop(BLK, (ITERS + 1) * BLK)
    def _(s):
        k, v = lax.div(s, BLK), lax.rem(s, BLK)
        others = (k * BLK - BLK, k * BLK)
        for r in range(len(rounds) + 1):

            @pl.when(s == BLK + r)
            def _(r=r):
                if r > 0:
                    knows(r - 1)
                if r < len(rounds):
                    tell(ready.at[r], *rounds[r])

        arrive_y(s - BLK)
        arrive_z(s - BLK, fast)
        apply(s, fast)

        @pl.when(s < ITERS * BLK)
        def _():
            send_z(s, fast)

        products(s, v, others, (fast,))
        arrive_z(s - BLK, core)
        apply(s, core)

        @pl.when(s < ITERS * BLK)
        def _():
            send_z(s, core)
            send_y(s)

        products(s, v, others, (core,), True)
        place(0, 2 * k - 1, v)
        place(1, 2 * k, v)
        split(k - 1, v)

    def copy(stage, i):
        partner, _, me, base = stage
        return pltpu.make_async_remote_copy(
            src_ref=gathered.at[base + me],
            dst_ref=gathered.at[base + me],
            send_sem=all_send.at[base + i],
            recv_sem=all_recv.at[base + i],
            device_id=partner(i),
            device_id_type=MESH,
        )

    total = moments[...]
    for stage in stages:
        _, size, me, base = stage
        gathered[base + me] = total
        for i in range(1, size):
            copy(stage, i).start()
        for i in range(1, size):
            copy(stage, i).wait_recv()
        total = gathered[base]
        for i in range(1, size):
            total = total + gathered[base + i]

    sum_ref[...] = total
    weights = weights_of(total)
    eighth, within = lax.div(lanes, 8), lax.rem(lanes, 8)
    for i in range(0, BLK, 2):
        wide = []
        for at in (i, i + 1):
            column = [lane(weights[h], at) for h in range(ITERS)]
            front = jnp.where(eighth == sub, column[0], 0.0) + jnp.where(
                eighth == sub + 8, column[1], 0.0
            )
            back = jnp.where(eighth == sub, column[2], 0.0)
            wide.append(
                [
                    jnp.where(within == sub, jnp.sum(part, axis=0, keepdims=True), 0.0)
                    for part in (front, back)
                ]
            )
        for part, (start, stop) in enumerate(((0, 128), (128, 8 * BLK * ITERS))):
            both = jnp.concatenate([wide[0][part], wide[1][part]], axis=0)
            high = both.astype(jnp.bfloat16)
            low = (both - high.astype(jnp.float32)).astype(jnp.bfloat16)
            mix_ref[8 * i : 8 * i + 16, start:stop] = high[:, : stop - start]
            mix_ref[64 + 8 * i : 64 + 8 * i + 16, start:stop] = low[:, : stop - start]
    @pl.loop(0, ITERS * BLK)
    def _(s):
        z_copy(s, fast).wait_send()

        @pl.when(off_chip)
        def _():
            z_copy(s, core).wait_send()

        for up in (0, 1):

            @pl.when(has_y[up])
            def _(up=up):
                y_copy(s, up).wait_send()

    for stage in stages:
        for i in range(1, stage[1]):
            copy(stage, i).wait_send()


def combine(high_ref, low_ref, mix_ref, sum_ref, out_ref, hess_ref, result, hess, out_sem, hess_sem):
    tiles = high_ref.shape[0] // 2

    def store(n):
        where = (slice(None), n // tiles, pl.ds(8 * (n % tiles), 8))
        return pltpu.make_async_copy(result.at[where], out_ref.at[where], out_sem.at[n])

    for h, tile in enumerate(hessenberg_of(sum_ref[...])):
        hess[8 * h : 8 * h + 8, :] = tile[:, : hess.shape[1]]
    for n in range(2 * tiles):
        both = jnp.dot(mix_ref[...], high_ref[n], preferred_element_type=jnp.float32)
        rest = jnp.dot(mix_ref[:64], low_ref[n], preferred_element_type=jnp.float32)
        total = both[:64] + (both[64:] + rest)
        result[:, n // tiles, 8 * (n % tiles) : 8 * (n % tiles) + 8, :] = total.reshape(
            BLK, 8, total.shape[1]
        )
        store(n).start()
    copy = pltpu.make_async_copy(hess, hess_ref, hess_sem)
    copy.start()
    for n in range(2 * tiles):
        store(n).wait()
    copy.wait()


def solution(mesh):
    n_gz, n_gy = mesh.shape["gz"], mesh.shape["gy"]
    n_z = n_gz // (CORES * Y_CHIPS)
    partners = n_gy * Y_CHIPS + n_z * CORES

    def body(right_side, diagonal):
        layers, n_rows, n_cols = diagonal.shape
        powers = ITERS * BLK
        pieces = layers * n_rows // 8
        vmem = lambda *shape: pltpu.VMEM(shape, jnp.float32)
        dma = pltpu.SemaphoreType.DMA
        whole = pl.BlockSpec(memory_space=pltpu.VMEM)
        high, low, mix, moments = pl.pallas_call(
            functools.partial(kernel, n_gz, n_gy),
            out_shape=(
                jax.ShapeDtypeStruct((pieces, 8 * powers, n_cols), jnp.bfloat16),
                jax.ShapeDtypeStruct((pieces, 8 * powers, n_cols), jnp.bfloat16),
                jax.ShapeDtypeStruct((16 * BLK, 8 * powers), jnp.bfloat16),
                jax.ShapeDtypeStruct((8, 128), jnp.float32),
            ),
            in_specs=[pl.BlockSpec(memory_space=pltpu.HBM)] * 2,
            out_specs=(whole,) * 4,
            scratch_shapes=[
                vmem(powers + BLK, layers, n_rows + 2 * TOP, n_cols),
                vmem(powers, 2, n_rows, n_cols),
                vmem(powers, 2, layers, 1, n_cols),
                vmem(powers, 2, layers, 1, n_cols),
                vmem(layers, n_rows, n_cols),
                vmem(2, 8, 128),
                vmem(8, 128),
                vmem(partners, 8, 128),
                dma((BLK,)),
                dma,
                dma((powers, 2)),
                dma((powers, 2)),
                dma((powers, 2)),
                dma((powers, 2)),
                dma((partners,)),
                dma((partners,)),
                pltpu.SemaphoreType.REGULAR((16,)),
            ],
            compiler_params=pltpu.CompilerParams(
                collective_id=0, has_side_effects=True, vmem_limit_bytes=28 << 20
            ),
            name="block_gmres",
        )(*(pltpu.with_memory_space_constraint(a, pltpu.HBM) for a in (right_side, diagonal)))
        return pl.pallas_call(
            combine,
            out_shape=(
                jax.ShapeDtypeStruct(right_side.shape, jnp.float32),
                jax.ShapeDtypeStruct((powers, powers + BLK), jnp.float32),
            ),
            in_specs=[whole] * 4,
            out_specs=(pl.BlockSpec(memory_space=pltpu.HBM),) * 2,
            scratch_shapes=[
                vmem(*right_side.shape),
                vmem(powers, powers + BLK),
                dma((pieces,)),
                dma,
            ],
            compiler_params=pltpu.CompilerParams(vmem_limit_bytes=12 << 20),
            name="combine",
        )(high, low, mix, moments)

    placed = (P(None, "gz", "gy", None), P("gz", "gy", None))
    return jax.shard_map(
        body, mesh=mesh, in_specs=placed, out_specs=(placed[0], P()), check_vma=False
    )
```

```python
import functools

import jax
import jax.numpy as jnp
from jax import lax
from jax.experimental import pallas as pl
from jax.experimental.pallas import tpu as pltpu
from jax.sharding import PartitionSpec as P

MESH = pl.DeviceIdType.MESH
BLK = 8
ITERS = 3
SHIFT = 7.0
TOP = 8
Y_CHIPS = 4
CORES = 2


def iotas():
    return (
        lax.broadcasted_iota(jnp.int32, (8, 128), 0),
        lax.broadcasted_iota(jnp.int32, (8, 128), 1),
    )


def sublane(tile, at):
    return jnp.broadcast_to(tile[at : at + 1, :], (8, 128))


def lane(tile, at):
    return jnp.broadcast_to(tile[:, at : at + 1], (8, 128))


def rsqrt(value):
    guess = lax.rsqrt(value)
    return guess * (1.5 - 0.5 * value * guess * guess)


def weights_of(moments):
    sub, _ = iotas()
    one = pltpu.roll(moments, 128 - 8, 1)
    two = pltpu.roll(moments, 128 - 16, 1)
    squares = two + (2.0 * SHIFT) * one + (SHIFT * SHIFT) * moments
    right = one + SHIFT * moments
    x = [right if h == 0 else pltpu.roll(right, 128 - 8 * h, 1) for h in range(ITERS)]
    tiles = [[lane(squares, 8 * j + v) for v in range(8)] for j in range(2 * ITERS - 1)]
    rows = [[tiles[a + h][i] for h in range(ITERS)] for a in range(ITERS) for i in range(8)]
    size = 8 * ITERS
    for k in range(size):
        g, q = divmod(k, 8)
        column = rows[k]
        inverse = 1.0 / sublane(column[g], q)
        pivot = sublane(x[g], q) * inverse
        for h in range(ITERS):
            x[h] = x[h] - column[h] * pivot
        x[g] = jnp.where(sub == q, pivot, x[g])
        for r in range(k + 1, size):
            factor = sublane(column[r // 8], r % 8) * inverse
            rows[r] = [rows[r][h] - factor * column[h] for h in range(ITERS)]
            rows[r][g] = jnp.where(sub == q, factor, rows[r][g])
    return x


def hessenberg_of(moments):
    sub, lanes = iotas()
    tiles = [[lane(moments, 8 * j + v) for v in range(8)] for j in range(2 * ITERS + 1)]
    groups = ITERS + 1
    rows = [[tiles[a + h][i] for h in range(groups)] for a in range(groups) for i in range(8)]
    size = 8 * groups
    factor_of, scale_of = [], []
    for k in range(size):
        g, q = divmod(k, 8)
        scale = rsqrt(sublane(rows[k][g], q))
        column = [None if h < g else rows[k][h] * scale for h in range(groups)]
        column[g] = jnp.where(sub >= q, column[g], 0.0)
        factor_of.append(column)
        scale_of.append(scale)
        for r in range(k + 1, size):
            factor = sublane(column[r // 8], r % 8)
            for h in range(r // 8, groups):
                rows[r][h] = rows[r][h] - factor * column[h]
    x = []
    for h in range(ITERS):
        tile = jnp.zeros((8, 128), jnp.float32)
        for c in range(8 * (h + 2)):
            tile = jnp.where(lanes == c, factor_of[c][h + 1], tile)
        x.append(tile)
    for k in range(8 * ITERS):
        g, q = divmod(k, 8)
        solved = sublane(x[g], q) * scale_of[k]
        for h in range(g, ITERS):
            x[h] = x[h] - factor_of[k][h] * solved
        x[g] = jnp.where(sub == q, solved, x[g])
    return [x[h] + jnp.where(lanes == 8 * h + sub, SHIFT, 0.0) for h in range(ITERS)]


def kernel(
    n_gz, n_gy, b_ref, d_ref, high_ref, low_ref, mix_ref, sum_ref,
    field, low_high, side_in, side_out, diag, rows_of, moments, gathered, last,
    load_sem, diag_sem, z_send, z_recv, y_send, y_recv, all_send, all_recv, ready, last_send, last_recv,
):
    gz, gy = lax.axis_index("gz"), lax.axis_index("gy")
    n_rows, n_cols = d_ref.shape[1], d_ref.shape[2]
    tiles = n_rows // 8
    core = lax.rem(gz, CORES)
    y_at = lax.rem(lax.div(gz, CORES), Y_CHIPS)
    z_at = lax.div(gz, CORES * Y_CHIPS)
    n_z = n_gz // (CORES * Y_CHIPS)
    fast = 1 - core
    own = pl.ds(TOP, n_rows)
    sub, lanes = iotas()

    def load(v):
        return pltpu.make_async_copy(b_ref.at[v], field.at[v, :, own, :], load_sem.at[v])

    diag_copy = pltpu.make_async_copy(d_ref, diag, diag_sem)
    load(0).start()
    load(1).start()
    diag_copy.start()
    for v in range(2, BLK):
        load(v).start()

    def around(at, i, size):
        return at + i if i == 0 else jnp.where(at + i >= size, at + (i - size), at + i)

    def first(i):
        return (gz + (around(y_at, i // n_gy, Y_CHIPS) - y_at) * CORES, around(gy, i % n_gy, n_gy))

    def second(i):
        to = (around(z_at, i // CORES, n_z) - z_at) * CORES * Y_CHIPS
        return (gz + to + around(core, i % CORES, CORES) - core, gy)

    stages = (
        (first, Y_CHIPS * n_gy, y_at * n_gy + gy, 0),
        (second, n_z * CORES, z_at * CORES + core, Y_CHIPS * n_gy),
    )

    def tell(semaphore, gz_step, gy_step):
        count = 0
        for sign in (-1, 1):
            to_gz, to_gy = gz + sign * gz_step, gy + sign * gy_step
            there = jnp.logical_and(
                jnp.logical_and(to_gz >= 0, to_gz < n_gz), jnp.logical_and(to_gy >= 0, to_gy < n_gy)
            )

            @pl.when(there)
            def _(to_gz=to_gz, to_gy=to_gy):
                pl.semaphore_signal(
                    semaphore, inc=1, device_id=(to_gz, to_gy), device_id_type=MESH
                )

            count += jnp.where(there, 1, 0)
        return count

    barrier = pltpu.get_barrier_semaphore()
    expected = tell(barrier, 1, 0) + tell(barrier, 0, 1)

    def clear(where, buffer, side):
        @pl.when(where)
        def _():
            @pl.loop(0, ITERS * BLK)
            def _(s):
                buffer[s, side] = jnp.zeros(buffer.shape[2:], jnp.float32)

    clear(gz == 0, low_high, 0)
    clear(gz == n_gz - 1, low_high, 1)
    clear(gy == 0, side_in, 0)
    clear(gy == n_gy - 1, side_in, 1)
    moments[...] = jnp.zeros((8, 128), jnp.float32)

    off_chip = jnp.where(core == 0, gz > 0, gz < n_gz - 1)

    pl.semaphore_wait(barrier, expected)

    rounds = []
    step = 1
    while step < n_gz:
        rounds.append((step, 0))
        step *= 2
    rounds += [(0, 1)] * (n_gy - 1)

    def knows(r):
        gz_step, gy_step = rounds[r]
        count = 0
        for sign in (-1, 1):
            to_gz, to_gy = gz + sign * gz_step, gy + sign * gy_step
            there = jnp.logical_and(
                jnp.logical_and(to_gz >= 0, to_gz < n_gz), jnp.logical_and(to_gy >= 0, to_gy < n_gy)
            )
            count += jnp.where(there, 1, 0)
        pl.semaphore_wait(ready.at[r], count)

    def z_copy(s, up):
        return pltpu.make_async_remote_copy(
            src_ref=field.at[s, up, own, :],
            dst_ref=low_high.at[s, 1 - up],
            send_sem=z_send.at[s, up],
            recv_sem=z_recv.at[s, 1 - up],
            device_id=(gz + 2 * up - 1, gy),
            device_id_type=MESH,
        )

    def y_copy(s, up):
        return pltpu.make_async_remote_copy(
            src_ref=side_out.at[s, up],
            dst_ref=side_in.at[s, 1 - up],
            send_sem=y_send.at[s, up],
            recv_sem=y_recv.at[s, 1 - up],
            device_id=(gz, gy + 2 * up - 1),
            device_id_type=MESH,
        )

    has_y = (gy > 0, gy < n_gy - 1)

    def send_z(s, layer):
        if layer is fast:
            z_copy(s, fast).start()
        else:

            @pl.when(off_chip)
            def _():
                z_copy(s, core).start()

    def send_y(s):
        for layer in (0, 1):
            side_out[s, 0, layer] = field[s, layer, TOP : TOP + 1, :]
            side_out[s, 1, layer] = field[s, layer, TOP + n_rows - 1 : TOP + n_rows, :]
        for up in (0, 1):

            @pl.when(has_y[up])
            def _(up=up):
                y_copy(s, up).start()

    def arrive_y(s):
        for up in (0, 1):

            @pl.when(has_y[up])
            def _(up=up):
                y_copy(s, 1 - up).wait_recv()

        for layer in (0, 1):
            field[s, layer, TOP - 1 : TOP, :] = side_in[s, 0, layer]
            field[s, layer, TOP + n_rows : TOP + n_rows + 1, :] = side_in[s, 1, layer]

    def arrive_z(s, layer):
        if layer is fast:
            z_copy(s, core).wait_recv()
        else:

            @pl.when(off_chip)
            def _():
                z_copy(s, fast).wait_recv()

    lane_of_row = lax.broadcasted_iota(jnp.int32, (8, n_cols), 1)

    def apply(s, layer):
        f = s - BLK
        for t in range(tiles):
            low = TOP + 8 * t
            here = field[f, layer, low : low + 8, :]
            beside = field[f, layer, low - 1 : low + 7, :] + field[f, layer, low + 1 : low + 9, :]
            other = field[f, 1 - layer, low : low + 8, :]
            beside = beside + (other + low_high[f, layer, 8 * t : 8 * t + 8, :])
            left = jnp.where(lane_of_row == 0, 0.0, pltpu.roll(here, 1, 1))
            right = jnp.where(lane_of_row == n_cols - 1, 0.0, pltpu.roll(here, n_cols - 1, 1))
            field[s, layer, low : low + 8, :] = diag[layer, 8 * t : 8 * t + 8, :] * here - (
                beside + (left + right)
            )

    def fold(row):
        total = row[:, :128]
        for at in range(128, n_cols, 128):
            total = total + row[:, at : at + 128]
        return jnp.sum(total, axis=0, keepdims=True)

    def products(s, v, others, layers, more=False):
        @pl.loop(0, v + 1)
        def _(u):
            totals = [jnp.zeros((8, n_cols), jnp.float32) for _ in others]
            for layer in layers:
                for t in range(tiles):
                    low = TOP + 8 * t
                    here = field[s, layer, low : low + 8, :]
                    totals = [
                        total + here * field[u + other, layer, low : low + 8, :]
                        for total, other in zip(totals, others)
                    ]
            for at, total in enumerate(totals):
                new = fold(total)
                if more:
                    new = new + rows_of[at, pl.ds(u, 1), :]
                rows_of[at, pl.ds(u, 1), :] = new

    def place(at, j, v):
        values = jnp.sum(rows_of[at], axis=1, keepdims=True)
        values = jnp.where(sub <= v, values, 0.0)
        new = jnp.where(lanes == j * 8 + v, values, 0.0)
        turned = jnp.where(jnp.logical_and(lanes == j * 8 + sub, sub < v), values, 0.0)
        turned = jnp.sum(turned, axis=0, keepdims=True)
        moments[...] = moments[...] + (new + jnp.where(sub == v, turned, 0.0))

    def split(k, part):
        for layer in (0, 1):
            low = pl.multiple_of(TOP + 8 * part, 8)
            values = field[pl.ds(k * BLK, BLK), layer, pl.ds(low, 8), :].reshape(8 * BLK, n_cols)
            high = values.astype(jnp.bfloat16)
            to = pl.ds(pl.multiple_of(k * (8 * BLK), 8 * BLK), 8 * BLK)
            high_ref[layer * tiles + part, to, :] = high
            low_ref[layer * tiles + part, to, :] = (values - high.astype(jnp.float32)).astype(
                jnp.bfloat16
            )

    rows_of[...] = jnp.zeros(rows_of.shape, jnp.float32)

    @pl.loop(0, BLK)
    def _(v):
        load(v).wait()
        send_z(v, core)
        send_z(v, fast)
        send_y(v)

    @pl.loop(0, BLK)
    def _(v):
        products(v, v, (0,), (0, 1))
        place(0, 0, v)

    diag_copy.wait()
    diag[...] = diag[...] + (6.0 - SHIFT)

    end = (ITERS + 1) * BLK - 1

    def advance(s, k, v):
        others = (k * BLK - BLK, k * BLK)
        arrive_y(s - BLK)
        arrive_z(s - BLK, fast)
        apply(s, fast)
        if s is not end:

            @pl.when(s < ITERS * BLK)
            def _():
                send_z(s, fast)

        products(s, v, others, (fast,))
        arrive_z(s - BLK, core)
        apply(s, core)
        if s is not end:

            @pl.when(s < ITERS * BLK)
            def _():
                send_z(s, core)
                send_y(s)

        products(s, v, others, (core,), True)

    @pl.loop(BLK, end)
    def _(s):
        k, v = lax.div(s, BLK), lax.rem(s, BLK)
        for r in range(len(rounds) + 1):

            @pl.when(s == BLK + r)
            def _(r=r):
                if r > 0:
                    knows(r - 1)
                if r < len(rounds):
                    tell(ready.at[r], *rounds[r])

        advance(s, k, v)
        place(0, 2 * k - 1, v)
        place(1, 2 * k, v)
        split(k - 1, v)

    def copy(stage, i):
        partner, _, me, base = stage
        return pltpu.make_async_remote_copy(
            src_ref=gathered.at[base + me],
            dst_ref=gathered.at[base + me],
            send_sem=all_send.at[base + i],
            recv_sem=all_recv.at[base + i],
            device_id=partner(i),
            device_id_type=MESH,
        )

    def start(stage, total):
        _, size, me, base = stage
        gathered[base + me] = total
        for i in range(1, size):
            copy(stage, i).start()

    def finish(stage):
        _, size, me, base = stage
        for i in range(1, size):
            copy(stage, i).wait_recv()
        total = gathered[base]
        for i in range(1, size):
            total = total + gathered[base + i]
        return total

    split(ITERS - 1, BLK - 1)
    start(stages[0], moments[...])
    advance(end, ITERS, BLK - 1)

    halves = [jnp.sum(rows_of[at], axis=1, keepdims=True) for at in (0, 1)]
    row = jnp.where(lanes == sub, halves[0], 0.0) + jnp.where(lanes == 8 + sub, halves[1], 0.0)
    here = gz * n_gy + gy
    last[here] = jnp.sum(row, axis=0, keepdims=True)
    zs = [around(z_at, i, n_z) * (CORES * Y_CHIPS) for i in range(n_z)]
    ys = [around(y_at, i, Y_CHIPS) * CORES for i in range(Y_CHIPS)]
    xs = [around(gy, i, n_gy) for i in range(n_gy)]
    cores = [core, fast]
    far = lambda i, size: min(i, size - i)
    others = [
        (-(far(a, n_z) + far(b, Y_CHIPS) + far(c, n_gy)), -d, a, b, c)
        for a in range(n_z) for b in range(Y_CHIPS) for c in range(n_gy) for d in range(CORES)
        if a + b + c + d
    ]

    def last_copy(source, device):
        return pltpu.make_async_remote_copy(
            src_ref=source,
            dst_ref=source,
            send_sem=last_send,
            recv_sem=last_recv,
            device_id=device,
            device_id_type=MESH,
        )

    for _, d, a, b, c in sorted(others):
        last_copy(last.at[here], (zs[a] + ys[b] + cores[-d], xs[c])).start()
    start(stages[1], finish(stages[0]))

    @pl.loop(0, ITERS * BLK)
    def _(s):
        z_copy(s, fast).wait_send()

        @pl.when(off_chip)
        def _():
            z_copy(s, core).wait_send()

        for up in (0, 1):

            @pl.when(has_y[up])
            def _(up=up):
                y_copy(s, up).wait_send()

    for stage in stages:
        for i in range(1, stage[1]):
            copy(stage, i).wait_send()
    everyone = last_copy(last.at[pl.ds(0, len(others))], (gz, gy))
    everyone.wait_send()
    total = finish(stages[1])
    everyone.wait_recv()
    sums = [last[i] for i in range(8)]
    for i in range(8, n_gz * n_gy):
        sums[i % 8] = sums[i % 8] + last[i]
    while len(sums) > 1:
        sums = [a + b for a, b in zip(sums[::2], sums[1::2])]
    final = jnp.broadcast_to(sums[0], (8, 128))
    at = 8 * (2 * ITERS - 1)
    total = total + jnp.where(
        jnp.logical_and(sub == 7, jnp.logical_and(lanes >= at, lanes < at + 16)),
        pltpu.roll(final, at, 1),
        0.0,
    )
    for n in (0, 1):
        column = jnp.sum(jnp.where(lanes == 8 * n + sub, final, 0.0), axis=1, keepdims=True)
        total = total + jnp.where(
            jnp.logical_and(sub < 7, lanes == at + 8 * n + 7), column, 0.0
        )

    sum_ref[...] = total
    weights = weights_of(total)
    eighth, within = lax.div(lanes, 8), lax.rem(lanes, 8)
    for i in range(0, BLK, 2):
        wide = []
        for at in (i, i + 1):
            column = [lane(weights[h], at) for h in range(ITERS)]
            front = jnp.where(eighth == sub, column[0], 0.0) + jnp.where(
                eighth == sub + 8, column[1], 0.0
            )
            back = jnp.where(eighth == sub, column[2], 0.0)
            wide.append(
                [
                    jnp.where(within == sub, jnp.sum(part, axis=0, keepdims=True), 0.0)
                    for part in (front, back)
                ]
            )
        for part, (start, stop) in enumerate(((0, 128), (128, 8 * BLK * ITERS))):
            both = jnp.concatenate([wide[0][part], wide[1][part]], axis=0)
            high = both.astype(jnp.bfloat16)
            low = (both - high.astype(jnp.float32)).astype(jnp.bfloat16)
            mix_ref[8 * i : 8 * i + 16, start:stop] = high[:, : stop - start]
            mix_ref[64 + 8 * i : 64 + 8 * i + 16, start:stop] = low[:, : stop - start]


def combine(high_ref, low_ref, mix_ref, sum_ref, out_ref, hess_ref, result, hess, out_sem, hess_sem):
    tiles = high_ref.shape[0] // 2

    def store(n):
        where = (slice(None), n // tiles, pl.ds(8 * (n % tiles), 8))
        return pltpu.make_async_copy(result.at[where], out_ref.at[where], out_sem.at[n])

    for h, tile in enumerate(hessenberg_of(sum_ref[...])):
        hess[8 * h : 8 * h + 8, :] = tile[:, : hess.shape[1]]
    for n in range(2 * tiles):
        both = jnp.dot(mix_ref[...], high_ref[n], preferred_element_type=jnp.float32)
        rest = jnp.dot(mix_ref[:64], low_ref[n], preferred_element_type=jnp.float32)
        total = both[:64] + (both[64:] + rest)
        result[:, n // tiles, 8 * (n % tiles) : 8 * (n % tiles) + 8, :] = total.reshape(
            BLK, 8, total.shape[1]
        )
        store(n).start()
    copy = pltpu.make_async_copy(hess, hess_ref, hess_sem)
    copy.start()
    for n in range(2 * tiles):
        store(n).wait()
    copy.wait()


def solution(mesh):
    n_gz, n_gy = mesh.shape["gz"], mesh.shape["gy"]
    n_z = n_gz // (CORES * Y_CHIPS)
    partners = n_gy * Y_CHIPS + n_z * CORES

    def body(right_side, diagonal):
        layers, n_rows, n_cols = diagonal.shape
        powers = ITERS * BLK
        pieces = layers * n_rows // 8
        vmem = lambda *shape: pltpu.VMEM(shape, jnp.float32)
        dma = pltpu.SemaphoreType.DMA
        whole = pl.BlockSpec(memory_space=pltpu.VMEM)
        high, low, mix, moments = pl.pallas_call(
            functools.partial(kernel, n_gz, n_gy),
            out_shape=(
                jax.ShapeDtypeStruct((pieces, 8 * powers, n_cols), jnp.bfloat16),
                jax.ShapeDtypeStruct((pieces, 8 * powers, n_cols), jnp.bfloat16),
                jax.ShapeDtypeStruct((16 * BLK, 8 * powers), jnp.bfloat16),
                jax.ShapeDtypeStruct((8, 128), jnp.float32),
            ),
            in_specs=[pl.BlockSpec(memory_space=pltpu.HBM)] * 2,
            out_specs=(whole,) * 4,
            scratch_shapes=[
                vmem(powers + BLK, layers, n_rows + 2 * TOP, n_cols),
                vmem(powers, 2, n_rows, n_cols),
                vmem(powers, 2, layers, 1, n_cols),
                vmem(powers, 2, layers, 1, n_cols),
                vmem(layers, n_rows, n_cols),
                vmem(2, 8, 128),
                vmem(8, 128),
                vmem(partners, 8, 128),
                vmem(n_gz * n_gy, 1, 128),
                dma((BLK,)),
                dma,
                dma((powers, 2)),
                dma((powers, 2)),
                dma((powers, 2)),
                dma((powers, 2)),
                dma((partners,)),
                dma((partners,)),
                pltpu.SemaphoreType.REGULAR((16,)),
                dma,
                dma,
            ],
            compiler_params=pltpu.CompilerParams(
                collective_id=0, has_side_effects=True, vmem_limit_bytes=28 << 20
            ),
            name="block_gmres",
        )(*(pltpu.with_memory_space_constraint(a, pltpu.HBM) for a in (right_side, diagonal)))
        return pl.pallas_call(
            combine,
            out_shape=(
                jax.ShapeDtypeStruct(right_side.shape, jnp.float32),
                jax.ShapeDtypeStruct((powers, powers + BLK), jnp.float32),
            ),
            in_specs=[whole] * 4,
            out_specs=(pl.BlockSpec(memory_space=pltpu.HBM),) * 2,
            scratch_shapes=[
                vmem(*right_side.shape),
                vmem(powers, powers + BLK),
                dma((pieces,)),
                dma,
            ],
            compiler_params=pltpu.CompilerParams(vmem_limit_bytes=12 << 20),
            name="combine",
        )(high, low, mix, moments)

    placed = (P(None, "gz", "gy", None), P("gz", "gy", None))
    return jax.shard_map(
        body, mesh=mesh, in_specs=placed, out_specs=(placed[0], P()), check_vma=False
    )
```

```python
import functools

import jax
import jax.numpy as jnp
from jax import lax
from jax.experimental import pallas as pl
from jax.experimental.pallas import tpu as pltpu
from jax.sharding import PartitionSpec as P

MESH = pl.DeviceIdType.MESH
BLK = 8
ITERS = 3
SHIFT = 7.0
TOP = 8
Y_CHIPS = 4
CORES = 2
CHUNK = 4


def iotas():
    return (
        lax.broadcasted_iota(jnp.int32, (8, 128), 0),
        lax.broadcasted_iota(jnp.int32, (8, 128), 1),
    )


def sublane(tile, at):
    return jnp.broadcast_to(tile[at : at + 1, :], (8, 128))


def lane(tile, at):
    return jnp.broadcast_to(tile[:, at : at + 1], (8, 128))


def rsqrt(value):
    guess = lax.rsqrt(value)
    return guess * (1.5 - 0.5 * value * guess * guess)


def eliminate(x, rows, start, stop):
    sub, _ = iotas()
    for k in range(start, stop):
        g, q = divmod(k, 8)
        column = rows[k]
        inverse = 1.0 / sublane(column[g], q)
        pivot = sublane(x[g], q) * inverse
        for h in range(ITERS):
            x[h] = x[h] - column[h] * pivot
        x[g] = jnp.where(sub == q, pivot, x[g])
        for r in range(k + 1, len(rows)):
            factor = sublane(column[r // 8], r % 8) * inverse
            rows[r] = [rows[r][h] - factor * column[h] for h in range(ITERS)]
            rows[r][g] = jnp.where(sub == q, factor, rows[r][g])


def begin_weights(moments):
    one = pltpu.roll(moments, 128 - 8, 1)
    two = pltpu.roll(moments, 128 - 16, 1)
    squares = two + (2.0 * SHIFT) * one + (SHIFT * SHIFT) * moments
    right = one + SHIFT * moments
    x = [right if h == 0 else pltpu.roll(right, 128 - 8 * h, 1) for h in range(ITERS)]
    tiles = [[lane(squares, 8 * j + v) for v in range(8)] for j in range(2 * ITERS - 1)]
    rows = [[tiles[a + h][i] for h in range(ITERS)] for a in range(ITERS) for i in range(8)]
    eliminate(x, rows, 0, 8)
    return x, rows


def end_weights(x, rows, fifth, sixth):
    for v in range(8):
        rows[8 + v][2] = rows[8 + v][2] + fifth[v]
        rows[16 + v][1] = rows[16 + v][1] + fifth[v]
        rows[16 + v][2] = rows[16 + v][2] + (sixth[v] + (2.0 * SHIFT) * fifth[v])
    eliminate(x, rows, 8, 8 * ITERS)
    return x


def hessenberg_of(moments):
    sub, lanes = iotas()
    tiles = [[lane(moments, 8 * j + v) for v in range(8)] for j in range(2 * ITERS + 1)]
    groups = ITERS + 1
    rows = [[tiles[a + h][i] for h in range(groups)] for a in range(groups) for i in range(8)]
    size = 8 * groups
    factor_of, scale_of = [], []
    for k in range(size):
        g, q = divmod(k, 8)
        scale = rsqrt(sublane(rows[k][g], q))
        column = [None if h < g else rows[k][h] * scale for h in range(groups)]
        column[g] = jnp.where(sub >= q, column[g], 0.0)
        factor_of.append(column)
        scale_of.append(scale)
        for r in range(k + 1, size):
            factor = sublane(column[r // 8], r % 8)
            for h in range(r // 8, groups):
                rows[r][h] = rows[r][h] - factor * column[h]
    x = []
    for h in range(ITERS):
        tile = jnp.zeros((8, 128), jnp.float32)
        for c in range(8 * (h + 2)):
            tile = jnp.where(lanes == c, factor_of[c][h + 1], tile)
        x.append(tile)
    for k in range(8 * ITERS):
        g, q = divmod(k, 8)
        solved = sublane(x[g], q) * scale_of[k]
        for h in range(g, ITERS):
            x[h] = x[h] - factor_of[k][h] * solved
        x[g] = jnp.where(sub == q, solved, x[g])
    return [x[h] + jnp.where(lanes == 8 * h + sub, SHIFT, 0.0) for h in range(ITERS)]


def kernel(
    n_gz, n_gy, b_ref, d_ref, high_ref, low_ref, mix_ref, sum_ref,
    field, low_high, side_in, side_out, diag, rows_of, moments, latest, gathered, last,
    load_sem, diag_sem, z_send, z_recv, y_send, y_recv, all_send, all_recv, ready, last_send, last_recv,
):
    gz, gy = lax.axis_index("gz"), lax.axis_index("gy")
    n_rows, n_cols = d_ref.shape[1], d_ref.shape[2]
    tiles = n_rows // 8
    core = lax.rem(gz, CORES)
    y_at = lax.rem(lax.div(gz, CORES), Y_CHIPS)
    z_at = lax.div(gz, CORES * Y_CHIPS)
    n_z = n_gz // (CORES * Y_CHIPS)
    fast = 1 - core
    own = pl.ds(TOP, n_rows)
    sub, lanes = iotas()

    def partners(gz_step, gy_step):
        both = []
        for sign in (-1, 1):
            to_gz, to_gy = gz + sign * gz_step, gy + sign * gy_step
            there = jnp.logical_and(
                jnp.logical_and(to_gz >= 0, to_gz < n_gz), jnp.logical_and(to_gy >= 0, to_gy < n_gy)
            )
            both.append((there, (to_gz, to_gy)))
        return sum(jnp.where(there, 1, 0) for there, _ in both), both

    def tell(semaphore, gz_step, gy_step):
        count, both = partners(gz_step, gy_step)
        for there, device in both:

            @pl.when(there)
            def _(device=device):
                pl.semaphore_signal(semaphore, inc=1, device_id=device, device_id_type=MESH)

        return count

    barrier = pltpu.get_barrier_semaphore()
    expected = tell(barrier, 1, 0) + tell(barrier, 0, 1)

    def load(v):
        return pltpu.make_async_copy(b_ref.at[v], field.at[v, :, own, :], load_sem.at[v])

    diag_copy = pltpu.make_async_copy(d_ref, diag, diag_sem)
    load(0).start()
    load(1).start()
    diag_copy.start()
    for v in range(2, BLK):
        load(v).start()

    def around(at, i, size):
        return at + i if i == 0 else jnp.where(at + i >= size, at + (i - size), at + i)

    def over_yx(i):
        return (gz + (around(y_at, i // n_gy, Y_CHIPS) - y_at) * CORES, around(gy, i % n_gy, n_gy))

    def over_zc(i):
        to = (around(z_at, i // CORES, n_z) - z_at) * CORES * Y_CHIPS
        return (gz + to + around(core, i % CORES, CORES) - core, gy)

    stages = (
        (over_zc, n_z * CORES, z_at * CORES + core, Y_CHIPS * n_gy),
        (over_yx, Y_CHIPS * n_gy, y_at * n_gy + gy, 0),
    )

    def clear(where, at):
        @pl.when(where)
        def _():
            @pl.loop(0, ITERS * BLK)
            def _(s):
                buffer = at(s)
                buffer[...] = jnp.zeros(buffer.shape, jnp.float32)

    for side, z_edge, y_edge in ((0, 0, 0), (1, n_gz - 1, n_gy - 1)):
        clear(gz == z_edge, lambda s, side=side: low_high.at[s, side])
        clear(gy == y_edge, lambda s, side=side: side_in.at[side, s])
    moments[...] = jnp.zeros((8, 128), jnp.float32)
    latest[...] = jnp.zeros((8, 128), jnp.float32)

    off_chip = jnp.where(core == 0, gz > 0, gz < n_gz - 1)

    pl.semaphore_wait(barrier, expected)

    doublings = (n_gz - 1).bit_length()
    rounds = doublings + n_gy - 1

    def reach(r):
        gz_step = 1
        for i in range(1, doublings):
            gz_step = jnp.where(r == i, 2**i, gz_step)
        along_gz = r < doublings
        return jnp.where(along_gz, gz_step, 0), jnp.where(along_gz, 0, 1)

    def z_copy(s, up, size):
        return pltpu.make_async_remote_copy(
            src_ref=field.at[pl.ds(s, size), up, own, :],
            dst_ref=low_high.at[pl.ds(s, size), 1 - up],
            send_sem=z_send.at[s, up],
            recv_sem=z_recv.at[s, 1 - up],
            device_id=(gz + 2 * up - 1, gy),
            device_id_type=MESH,
        )

    def by_chunk(s, at_end, do):
        edge = CHUNK - 1 if at_end else 0
        if isinstance(s, int):
            if s < ITERS * BLK and s % CHUNK == edge:
                do(s - edge)
            return

        @pl.when(jnp.logical_and(s < ITERS * BLK, lax.rem(s, CHUNK) == edge))
        def _():
            do(s - edge)

    def y_copy(s, up):
        return pltpu.make_async_remote_copy(
            src_ref=side_out.at[up, pl.ds(s, CHUNK)],
            dst_ref=side_in.at[1 - up, pl.ds(s, CHUNK)],
            send_sem=y_send.at[s, up],
            recv_sem=y_recv.at[s, 1 - up],
            device_id=(gz, gy + 2 * up - 1),
            device_id_type=MESH,
        )

    has_y = (gy > 0, gy < n_gy - 1)

    def send_slow(s):
        @pl.when(off_chip)
        def _():
            z_copy(s, core, 1).start()

    def send_fast(s):
        for layer in (0, 1):
            side_out[0, s, layer] = field[s, layer, TOP : TOP + 1, :]
            side_out[1, s, layer] = field[s, layer, TOP + n_rows - 1 : TOP + n_rows, :]

        def start(at):
            z_copy(at, fast, CHUNK).start()
            for up in (0, 1):

                @pl.when(has_y[up])
                def _(up=up):
                    y_copy(at, up).start()

        by_chunk(s, True, start)

    def arrive_fast(s):
        def wait(at):
            z_copy(at, core, CHUNK).wait_recv()
            for up in (0, 1):

                @pl.when(has_y[up])
                def _(up=up):
                    y_copy(at, 1 - up).wait_recv()

        by_chunk(s, False, wait)
        for layer in (0, 1):
            field[s, layer, TOP - 1 : TOP, :] = side_in[0, s, layer]
            field[s, layer, TOP + n_rows : TOP + n_rows + 1, :] = side_in[1, s, layer]

    def arrive_slow(s):
        @pl.when(off_chip)
        def _():
            z_copy(s, fast, 1).wait_recv()

    lane_of_row = lax.broadcasted_iota(jnp.int32, (8, n_cols), 1)

    def apply(s, layer, ghost=True):
        f = s - BLK
        for t in range(tiles):
            low = TOP + 8 * t
            here = field[f, layer, low : low + 8, :]
            beside = field[f, layer, low - 1 : low + 7, :] + field[f, layer, low + 1 : low + 9, :]
            other = field[f, 1 - layer, low : low + 8, :]
            if ghost:
                other = other + low_high[f, layer, 8 * t : 8 * t + 8, :]
            beside = beside + other
            left = jnp.where(lane_of_row == 0, 0.0, pltpu.roll(here, 1, 1))
            right = jnp.where(lane_of_row == n_cols - 1, 0.0, pltpu.roll(here, n_cols - 1, 1))
            field[s, layer, low : low + 8, :] = diag[layer, 8 * t : 8 * t + 8, :] * here - (
                beside + (left + right)
            )

    def fold(row):
        total = row[:, :128]
        for at in range(128, n_cols, 128):
            total = total + row[:, at : at + 128]
        return jnp.sum(total, axis=0, keepdims=True)

    def products(s, v, others, layers, more=False):
        def block(u, size):
            totals = [jnp.zeros((8, n_cols), jnp.float32) for _ in range(size * len(others))]
            for layer in layers:
                for t in range(tiles):
                    low = TOP + 8 * t
                    here = field[s, layer, low : low + 8, :]
                    totals = [
                        total + here * field[u + n % size + others[n // size], layer, low : low + 8, :]
                        for n, total in enumerate(totals)
                    ]
            for n, total in enumerate(totals):
                new = fold(total)
                to = pl.ds(u + n % size, 1)
                if more:
                    new = new + rows_of[n // size, to, :]
                rows_of[n // size, to, :] = new

        pairs = lax.div(v + 1, 2)

        @pl.loop(0, pairs)
        def _(n):
            block(2 * n, 2)

        @pl.when(lax.rem(v, 2) == 0)
        def _():
            block(v, 1)

    def place(which, v):
        change = jnp.zeros((8, 128), jnp.float32)
        turned = jnp.zeros((8, 128), jnp.float32)
        for at, j in which:
            values = jnp.sum(rows_of[at], axis=1, keepdims=True)
            change = change + jnp.where(
                jnp.logical_and(sub <= v, lanes == j * 8 + v), values, 0.0
            )
            turned = turned + jnp.where(
                jnp.logical_and(lanes == j * 8 + sub, sub < v), values, 0.0
            )
        turned = jnp.sum(turned, axis=0, keepdims=True)
        moments[...] = moments[...] + (change + jnp.where(sub == v, turned, 0.0))

    def place_latest(v):
        change = jnp.zeros((8, 128), jnp.float32)
        for at in (0, 1):
            values = jnp.sum(rows_of[at], axis=1, keepdims=True)
            change = change + jnp.where(
                jnp.logical_or(
                    jnp.logical_and(sub <= v, lanes == 16 * sub + (8 * at + v)),
                    jnp.logical_and(sub < v, lanes == 16 * v + 8 * at + sub),
                ),
                values,
                0.0,
            )
        latest[...] = latest[...] + change

    def split(k, part):
        for layer in (0, 1):
            low = pl.multiple_of(TOP + 8 * part, 8)
            values = field[pl.ds(k * BLK, BLK), layer, pl.ds(low, 8), :].reshape(8 * BLK, n_cols)
            high = values.astype(jnp.bfloat16)
            to = pl.ds(pl.multiple_of(k * (8 * BLK), 8 * BLK), 8 * BLK)
            high_ref[layer * tiles + part, to, :] = high
            low_ref[layer * tiles + part, to, :] = (values - high.astype(jnp.float32)).astype(
                jnp.bfloat16
            )

    rows_of[...] = jnp.zeros(rows_of.shape, jnp.float32)

    @pl.loop(0, BLK)
    def _(v):
        load(v).wait()

        send_slow(v)
        send_fast(v)

    @pl.loop(0, BLK)
    def _(v):
        products(v, v, (0,), (0, 1))
        place([(0, 0)], v)

    diag_copy.wait()
    diag[...] = diag[...] + (6.0 - SHIFT)

    def copy(stage, i):
        partner, _, me, base = stage
        return pltpu.make_async_remote_copy(
            src_ref=gathered.at[base + me],
            dst_ref=gathered.at[base + me],
            send_sem=all_send.at[base + i],
            recv_sem=all_recv.at[base + i],
            device_id=partner(i),
            device_id_type=MESH,
        )

    def start(stage, total):
        _, size, me, base = stage
        gathered[base + me] = total
        for i in range(1, size):
            copy(stage, i).start()

    def finish(stage):
        _, size, me, base = stage
        for i in range(1, size):
            copy(stage, i).wait_recv()
        total = gathered[base]
        for i in range(1, size):
            total = total + gathered[base + i]
        return total

    end = (ITERS + 1) * BLK - 1

    def advance(s, k, v):
        others = (k * BLK - BLK, k * BLK)
        arrive_fast(s - BLK)
        apply(s, fast)
        products(s, v, others, (fast,))
        arrive_slow(s - BLK)
        apply(s, core)

        @pl.when(s < ITERS * BLK)
        def _():
            send_slow(s)
            send_fast(s)

        products(s, v, others, (core,), True)

    def advance_last():
        s, v = end, BLK - 1
        others = (s - v - BLK, s - v)
        arrive_fast(s - BLK)
        apply(s, fast)
        products(s, v, others, (fast,))
        apply(s, core, ghost=False)
        products(s, v, others, (core,), True)
        arrive_slow(s - BLK)

        def block(u, holds_last):
            totals = [jnp.zeros((8, n_cols), jnp.float32) for _ in range(4)]
            for t in range(tiles):
                low = TOP + 8 * t
                ghost = low_high[s - BLK, core, 8 * t : 8 * t + 8, :]
                for n in range(4):
                    field_of = field[u + n % 2 + others[n // 2], core, low : low + 8, :]
                    if holds_last and n == 3:
                        field_of = 2.0 * field_of - ghost
                    totals[n] = totals[n] + ghost * field_of
            for n, total in enumerate(totals):
                to = pl.ds(u + n % 2, 1)
                rows_of[n // 2, to, :] = rows_of[n // 2, to, :] - fold(total)

        @pl.loop(0, BLK // 2 - 1)
        def _(n):
            block(2 * n, False)

        block(BLK - 2, True)

    @pl.loop(BLK, end)
    def _(s):
        k, v = lax.div(s, BLK), lax.rem(s, BLK)

        @pl.when(s <= BLK + rounds)
        def _():
            r = s - BLK

            @pl.when(r > 0)
            def _():
                pl.semaphore_wait(ready.at[r - 1], partners(*reach(r - 1))[0])

            @pl.when(r < rounds)
            def _():
                tell(ready.at[r], *reach(r))

        @pl.when(s == ITERS * BLK)
        def _():
            start(stages[0], moments[...])

        advance(s, k, v)

        @pl.when(k < ITERS)
        def _():
            place([(0, 2 * k - 1), (1, 2 * k)], v)

        @pl.when(k == ITERS)
        def _():
            place_latest(v)

        split(k - 1, v)

    advance_last()
    place_latest(BLK - 1)

    here = gz * n_gy + gy
    last[here] = jnp.sum(latest[...], axis=0, keepdims=True)
    zs = [around(z_at, i, n_z) * (CORES * Y_CHIPS) for i in range(n_z)]
    ys = [around(y_at, i, Y_CHIPS) * CORES for i in range(Y_CHIPS)]
    xs = [around(gy, i, n_gy) for i in range(n_gy)]
    cores = [core, fast]
    far = lambda i, size: min(i, size - i)
    others = [
        (-(far(a, n_z) + far(b, Y_CHIPS) + far(c, n_gy)), -d, a, b, c)
        for a in range(n_z) for b in range(Y_CHIPS) for c in range(n_gy) for d in range(CORES)
        if a + b + c + d
    ]

    def last_copy(source, device):
        return pltpu.make_async_remote_copy(
            src_ref=source,
            dst_ref=source,
            send_sem=last_send,
            recv_sem=last_recv,
            device_id=device,
            device_id_type=MESH,
        )

    for _, d, a, b, c in sorted(others):
        last_copy(last.at[here], (zs[a] + ys[b] + cores[-d], xs[c])).start()
    start(stages[1], finish(stages[0]))
    split(ITERS - 1, BLK - 1)

    @pl.loop(0, ITERS * BLK)
    def _(s):
        @pl.when(off_chip)
        def _():
            z_copy(s, core, 1).wait_send()

    @pl.loop(0, ITERS * BLK // CHUNK)
    def _(n):
        z_copy(n * CHUNK, fast, CHUNK).wait_send()
        for up in (0, 1):

            @pl.when(has_y[up])
            def _(up=up):
                y_copy(n * CHUNK, up).wait_send()

    for stage in stages:
        for i in range(1, stage[1]):
            copy(stage, i).wait_send()
    everyone = last_copy(last.at[pl.ds(0, len(others))], (gz, gy))
    everyone.wait_send()
    total = finish(stages[1])
    x, rows = begin_weights(total)
    everyone.wait_recv()
    sums = [last[i] for i in range(8)]
    for i in range(8, n_gz * n_gy):
        sums[i % 8] = sums[i % 8] + last[i]
    while len(sums) > 1:
        sums = [a + b for a, b in zip(sums[::2], sums[1::2])]
    final = jnp.broadcast_to(sums[0], (8, 128))
    tiles_of = [
        [
            jnp.broadcast_to(
                jnp.sum(
                    jnp.where(lanes == 16 * sub + (8 * at + v), final, 0.0), axis=1, keepdims=True
                ),
                (8, 128),
            )
            for v in range(BLK)
        ]
        for at in (0, 1)
    ]
    for at in (0, 1):
        for v in range(BLK):
            total = jnp.where(lanes == 8 * (2 * ITERS - 1 + at) + v, tiles_of[at][v], total)

    sum_ref[...] = total
    weights = end_weights(x, rows, *tiles_of)
    eighth, within = lax.div(lanes, 8), lax.rem(lanes, 8)
    for i in range(0, BLK, 2):
        wide = []
        for at in (i, i + 1):
            column = [lane(weights[h], at) for h in range(ITERS)]
            front = jnp.where(eighth == sub, column[0], 0.0) + jnp.where(
                eighth == sub + 8, column[1], 0.0
            )
            back = jnp.where(eighth == sub, column[2], 0.0)
            wide.append(
                [
                    jnp.where(within == sub, jnp.sum(part, axis=0, keepdims=True), 0.0)
                    for part in (front, back)
                ]
            )
        for part, (start, stop) in enumerate(((0, 128), (128, 8 * BLK * ITERS))):
            both = jnp.concatenate([wide[0][part], wide[1][part]], axis=0)
            high = both.astype(jnp.bfloat16)
            low = (both - high.astype(jnp.float32)).astype(jnp.bfloat16)
            mix_ref[8 * i : 8 * i + 16, start:stop] = high[:, : stop - start]
            mix_ref[64 + 8 * i : 64 + 8 * i + 16, start:stop] = low[:, : stop - start]


def combine(high_ref, low_ref, mix_ref, sum_ref, out_ref, hess_ref, result, hess, out_sem, hess_sem):
    tiles = high_ref.shape[0] // 2

    def store(n):
        where = (slice(None), n // tiles, pl.ds(8 * (n % tiles), 8))
        return pltpu.make_async_copy(result.at[where], out_ref.at[where], out_sem.at[n])

    for h, tile in enumerate(hessenberg_of(sum_ref[...])):
        hess[8 * h : 8 * h + 8, :] = tile[:, : hess.shape[1]]
    for n in range(2 * tiles):
        both = jnp.dot(mix_ref[...], high_ref[n], preferred_element_type=jnp.float32)
        rest = jnp.dot(mix_ref[:64], low_ref[n], preferred_element_type=jnp.float32)
        total = both[:64] + (both[64:] + rest)
        result[:, n // tiles, 8 * (n % tiles) : 8 * (n % tiles) + 8, :] = total.reshape(
            BLK, 8, total.shape[1]
        )
        store(n).start()
    copy = pltpu.make_async_copy(hess, hess_ref, hess_sem)
    copy.start()
    for n in range(2 * tiles):
        store(n).wait()
    copy.wait()


def solution(mesh):
    n_gz, n_gy = mesh.shape["gz"], mesh.shape["gy"]
    n_z = n_gz // (CORES * Y_CHIPS)
    partners = n_gy * Y_CHIPS + n_z * CORES

    def body(right_side, diagonal):
        layers, n_rows, n_cols = diagonal.shape
        powers = ITERS * BLK
        pieces = layers * n_rows // 8
        vmem = lambda *shape: pltpu.VMEM(shape, jnp.float32)
        dma = pltpu.SemaphoreType.DMA
        whole = pl.BlockSpec(memory_space=pltpu.VMEM)
        high, low, mix, moments = pl.pallas_call(
            functools.partial(kernel, n_gz, n_gy),
            out_shape=(
                jax.ShapeDtypeStruct((pieces, 8 * powers, n_cols), jnp.bfloat16),
                jax.ShapeDtypeStruct((pieces, 8 * powers, n_cols), jnp.bfloat16),
                jax.ShapeDtypeStruct((16 * BLK, 8 * powers), jnp.bfloat16),
                jax.ShapeDtypeStruct((8, 128), jnp.float32),
            ),
            in_specs=[pl.BlockSpec(memory_space=pltpu.HBM)] * 2,
            out_specs=(whole,) * 4,
            scratch_shapes=[
                vmem(powers + BLK, layers, n_rows + 2 * TOP, n_cols),
                vmem(powers, 2, n_rows, n_cols),
                vmem(2, powers, layers, 1, n_cols),
                vmem(2, powers, layers, 1, n_cols),
                vmem(layers, n_rows, n_cols),
                vmem(2, 8, 128),
                vmem(8, 128),
                vmem(8, 128),
                vmem(partners, 8, 128),
                vmem(n_gz * n_gy, 1, 128),
                dma((BLK,)),
                dma,
                dma((powers, 2)),
                dma((powers, 2)),
                dma((powers, 2)),
                dma((powers, 2)),
                dma((partners,)),
                dma((partners,)),
                pltpu.SemaphoreType.REGULAR((16,)),
                dma,
                dma,
            ],
            compiler_params=pltpu.CompilerParams(
                collective_id=0, has_side_effects=True, vmem_limit_bytes=28 << 20
            ),
            name="block_gmres",
        )(*(pltpu.with_memory_space_constraint(a, pltpu.HBM) for a in (right_side, diagonal)))
        return pl.pallas_call(
            combine,
            out_shape=(
                jax.ShapeDtypeStruct(right_side.shape, jnp.float32),
                jax.ShapeDtypeStruct((powers, powers + BLK), jnp.float32),
            ),
            in_specs=[whole] * 4,
            out_specs=(pl.BlockSpec(memory_space=pltpu.HBM),) * 2,
            scratch_shapes=[
                vmem(*right_side.shape),
                vmem(powers, powers + BLK),
                dma((pieces,)),
                dma,
            ],
            compiler_params=pltpu.CompilerParams(vmem_limit_bytes=12 << 20),
            name="combine",
        )(high, low, mix, moments)

    placed = (P(None, "gz", "gy", None), P("gz", "gy", None))
    return jax.shard_map(
        body, mesh=mesh, in_specs=placed, out_specs=(placed[0], P()), check_vma=False
    )
```

```python
import functools

import jax
import jax.numpy as jnp
from jax import lax
from jax.experimental import pallas as pl
from jax.experimental.pallas import tpu as pltpu
from jax.sharding import PartitionSpec as P

MESH = pl.DeviceIdType.MESH
BLK = 8
ITERS = 3
SHIFT = 7.0
TOP = 8
Y_CHIPS = 4
CORES = 2
CHUNK = 4


def iotas():
    return (
        lax.broadcasted_iota(jnp.int32, (8, 128), 0),
        lax.broadcasted_iota(jnp.int32, (8, 128), 1),
    )


def sublane(tile, at):
    return jnp.broadcast_to(tile[at : at + 1, :], (8, 128))


def lane(tile, at):
    return jnp.broadcast_to(tile[:, at : at + 1], (8, 128))


def rsqrt(value):
    guess = lax.rsqrt(value)
    return guess * (1.5 - 0.5 * value * guess * guess)


def eliminate(x, rows, start, stop):
    sub, _ = iotas()
    for k in range(start, stop):
        g, q = divmod(k, 8)
        column = rows[k]
        inverse = 1.0 / sublane(column[g], q)
        pivot = sublane(x[g], q) * inverse
        for h in range(ITERS):
            x[h] = x[h] - column[h] * pivot
        x[g] = jnp.where(sub == q, pivot, x[g])
        for r in range(k + 1, len(rows)):
            factor = sublane(column[r // 8], r % 8) * inverse
            rows[r] = [rows[r][h] - factor * column[h] for h in range(ITERS)]
            rows[r][g] = jnp.where(sub == q, factor, rows[r][g])


def begin_weights(moments):
    one = pltpu.roll(moments, 128 - 8, 1)
    two = pltpu.roll(moments, 128 - 16, 1)
    squares = two + (2.0 * SHIFT) * one + (SHIFT * SHIFT) * moments
    right = one + SHIFT * moments
    x = [right if h == 0 else pltpu.roll(right, 128 - 8 * h, 1) for h in range(ITERS)]
    tiles = [[lane(squares, 8 * j + v) for v in range(8)] for j in range(2 * ITERS - 1)]
    rows = [[tiles[a + h][i] for h in range(ITERS)] for a in range(ITERS) for i in range(8)]
    eliminate(x, rows, 0, 8)
    return x, rows


def end_weights(x, rows, fifth, sixth):
    for v in range(8):
        rows[8 + v][2] = rows[8 + v][2] + fifth[v]
        rows[16 + v][1] = rows[16 + v][1] + fifth[v]
        rows[16 + v][2] = rows[16 + v][2] + (sixth[v] + (2.0 * SHIFT) * fifth[v])
    eliminate(x, rows, 8, 8 * ITERS)
    return x


def hessenberg_of(moments):
    sub, lanes = iotas()
    tiles = [[lane(moments, 8 * j + v) for v in range(8)] for j in range(2 * ITERS + 1)]
    groups = ITERS + 1
    rows = [[tiles[a + h][i] for h in range(groups)] for a in range(groups) for i in range(8)]
    size = 8 * groups
    factor_of, scale_of = [], []
    for k in range(size):
        g, q = divmod(k, 8)
        scale = rsqrt(sublane(rows[k][g], q))
        column = [None if h < g else rows[k][h] * scale for h in range(groups)]
        column[g] = jnp.where(sub >= q, column[g], 0.0)
        factor_of.append(column)
        scale_of.append(scale)
        for r in range(k + 1, size):
            factor = sublane(column[r // 8], r % 8)
            for h in range(r // 8, groups):
                rows[r][h] = rows[r][h] - factor * column[h]
    x = []
    for h in range(ITERS):
        tile = jnp.zeros((8, 128), jnp.float32)
        for c in range(8 * (h + 2)):
            tile = jnp.where(lanes == c, factor_of[c][h + 1], tile)
        x.append(tile)
    for k in range(8 * ITERS):
        g, q = divmod(k, 8)
        solved = sublane(x[g], q) * scale_of[k]
        for h in range(g, ITERS):
            x[h] = x[h] - factor_of[k][h] * solved
        x[g] = jnp.where(sub == q, solved, x[g])
    return [x[h] + jnp.where(lanes == 8 * h + sub, SHIFT, 0.0) for h in range(ITERS)]


def kernel(
    n_gz, n_gy, b_ref, d_ref, high_ref, low_ref, mix_ref, sum_ref,
    field, low_high, side_in, side_out, diag, rows_of, moments, latest, gathered, last,
    load_sem, diag_sem, z_send, z_recv, y_send, y_recv, all_send, all_recv, ready, last_send, last_recv,
):
    gz, gy = lax.axis_index("gz"), lax.axis_index("gy")
    n_rows, n_cols = d_ref.shape[1], d_ref.shape[2]
    tiles = n_rows // 8
    core = lax.rem(gz, CORES)
    y_at = lax.rem(lax.div(gz, CORES), Y_CHIPS)
    z_at = lax.div(gz, CORES * Y_CHIPS)
    n_z = n_gz // (CORES * Y_CHIPS)
    fast = 1 - core
    own = pl.ds(TOP, n_rows)
    sub, lanes = iotas()

    def partners(gz_step, gy_step):
        both = []
        for sign in (-1, 1):
            to_gz, to_gy = gz + sign * gz_step, gy + sign * gy_step
            there = jnp.logical_and(
                jnp.logical_and(to_gz >= 0, to_gz < n_gz), jnp.logical_and(to_gy >= 0, to_gy < n_gy)
            )
            both.append((there, (to_gz, to_gy)))
        return sum(jnp.where(there, 1, 0) for there, _ in both), both

    def tell(semaphore, gz_step, gy_step):
        count, both = partners(gz_step, gy_step)
        for there, device in both:

            @pl.when(there)
            def _(device=device):
                pl.semaphore_signal(semaphore, inc=1, device_id=device, device_id_type=MESH)

        return count

    barrier = pltpu.get_barrier_semaphore()
    expected = tell(barrier, 1, 0) + tell(barrier, 0, 1)

    def load(v):
        return pltpu.make_async_copy(b_ref.at[v], field.at[v, :, own, :], load_sem.at[v])

    diag_copy = pltpu.make_async_copy(d_ref, diag, diag_sem)
    load(0).start()
    load(1).start()
    diag_copy.start()
    for v in range(2, BLK):
        load(v).start()

    def around(at, i, size):
        return at + i if i == 0 else jnp.where(at + i >= size, at + (i - size), at + i)

    def over_yx(i):
        return (gz + (around(y_at, i // n_gy, Y_CHIPS) - y_at) * CORES, around(gy, i % n_gy, n_gy))

    def over_zc(i):
        to = (around(z_at, i // CORES, n_z) - z_at) * CORES * Y_CHIPS
        return (gz + to + around(core, i % CORES, CORES) - core, gy)

    stages = (
        (over_zc, n_z * CORES, z_at * CORES + core, Y_CHIPS * n_gy),
        (over_yx, Y_CHIPS * n_gy, y_at * n_gy + gy, 0),
    )

    def clear(where, at):
        @pl.when(where)
        def _():
            @pl.loop(0, ITERS * BLK)
            def _(s):
                buffer = at(s)
                buffer[...] = jnp.zeros(buffer.shape, jnp.float32)

    for side, z_edge, y_edge in ((0, 0, 0), (1, n_gz - 1, n_gy - 1)):
        clear(gz == z_edge, lambda s, side=side: low_high.at[s, side])
        clear(gy == y_edge, lambda s, side=side: side_in.at[side, s])
    moments[...] = jnp.zeros((8, 128), jnp.float32)
    latest[...] = jnp.zeros((8, 128), jnp.float32)

    off_chip = jnp.where(core == 0, gz > 0, gz < n_gz - 1)

    pl.semaphore_wait(barrier, expected)

    doublings = (n_gz - 1).bit_length()
    rounds = doublings + n_gy - 1

    def reach(r):
        gz_step = 1
        for i in range(1, doublings):
            gz_step = jnp.where(r == i, 2**i, gz_step)
        along_gz = r < doublings
        return jnp.where(along_gz, gz_step, 0), jnp.where(along_gz, 0, 1)

    def z_copy(s, up, size):
        return pltpu.make_async_remote_copy(
            src_ref=field.at[pl.ds(s, size), up, own, :],
            dst_ref=low_high.at[pl.ds(s, size), 1 - up],
            send_sem=z_send.at[s, up],
            recv_sem=z_recv.at[s, 1 - up],
            device_id=(gz + 2 * up - 1, gy),
            device_id_type=MESH,
        )

    def by_chunk(s, at_end, do):
        edge = CHUNK - 1 if at_end else 0
        if isinstance(s, int):
            if s < ITERS * BLK and s % CHUNK == edge:
                do(s - edge)
            return

        @pl.when(jnp.logical_and(s < ITERS * BLK, lax.rem(s, CHUNK) == edge))
        def _():
            do(s - edge)

    def y_copy(s, up):
        return pltpu.make_async_remote_copy(
            src_ref=side_out.at[up, pl.ds(s, CHUNK)],
            dst_ref=side_in.at[1 - up, pl.ds(s, CHUNK)],
            send_sem=y_send.at[s, up],
            recv_sem=y_recv.at[s, 1 - up],
            device_id=(gz, gy + 2 * up - 1),
            device_id_type=MESH,
        )

    has_y = (gy > 0, gy < n_gy - 1)

    last_sent = ITERS * BLK - 1
    half = n_rows // 2

    def half_copy(part, up):
        return pltpu.make_async_remote_copy(
            src_ref=field.at[last_sent, up, pl.ds(TOP + part * half, half), :],
            dst_ref=low_high.at[last_sent, 1 - up, pl.ds(part * half, half)],
            send_sem=z_send.at[last_sent + part, up],
            recv_sem=z_recv.at[last_sent + part, 1 - up],
            device_id=(gz + 2 * up - 1, gy),
            device_id_type=MESH,
        )

    def send_slow(s):
        @pl.when(jnp.logical_and(off_chip, s < last_sent))
        def _():
            z_copy(s, core, 1).start()

        @pl.when(jnp.logical_and(off_chip, s == last_sent))
        def _():
            half_copy(0, core).start()
            half_copy(1, core).start()

    def send_fast(s):
        for layer in (0, 1):
            side_out[0, s, layer] = field[s, layer, TOP : TOP + 1, :]
            side_out[1, s, layer] = field[s, layer, TOP + n_rows - 1 : TOP + n_rows, :]

        def start(at):
            z_copy(at, fast, CHUNK).start()
            for up in (0, 1):

                @pl.when(has_y[up])
                def _(up=up):
                    y_copy(at, up).start()

        by_chunk(s, True, start)

    def arrive_fast(s):
        def wait(at):
            z_copy(at, core, CHUNK).wait_recv()
            for up in (0, 1):

                @pl.when(has_y[up])
                def _(up=up):
                    y_copy(at, 1 - up).wait_recv()

        by_chunk(s, False, wait)
        for layer in (0, 1):
            field[s, layer, TOP - 1 : TOP, :] = side_in[0, s, layer]
            field[s, layer, TOP + n_rows : TOP + n_rows + 1, :] = side_in[1, s, layer]

    def arrive_slow(s):
        @pl.when(off_chip)
        def _():
            z_copy(s, fast, 1).wait_recv()

    lane_of_row = lax.broadcasted_iota(jnp.int32, (8, n_cols), 1)

    def apply(s, layer, ghost=True):
        f = s - BLK
        for t in range(tiles):
            low = TOP + 8 * t
            here = field[f, layer, low : low + 8, :]
            beside = field[f, layer, low - 1 : low + 7, :] + field[f, layer, low + 1 : low + 9, :]
            other = field[f, 1 - layer, low : low + 8, :]
            if ghost:
                other = other + low_high[f, layer, 8 * t : 8 * t + 8, :]
            beside = beside + other
            left = jnp.where(lane_of_row == 0, 0.0, pltpu.roll(here, 1, 1))
            right = jnp.where(lane_of_row == n_cols - 1, 0.0, pltpu.roll(here, n_cols - 1, 1))
            field[s, layer, low : low + 8, :] = diag[layer, 8 * t : 8 * t + 8, :] * here - (
                beside + (left + right)
            )

    def fold(row):
        total = row[:, :128]
        for at in range(128, n_cols, 128):
            total = total + row[:, at : at + 128]
        return jnp.sum(total, axis=0, keepdims=True)

    def products(s, v, others, layers, more=False):
        def block(u, size):
            totals = [jnp.zeros((8, n_cols), jnp.float32) for _ in range(size * len(others))]
            for layer in layers:
                for t in range(tiles):
                    low = TOP + 8 * t
                    here = field[s, layer, low : low + 8, :]
                    totals = [
                        total + here * field[u + n % size + others[n // size], layer, low : low + 8, :]
                        for n, total in enumerate(totals)
                    ]
            for n, total in enumerate(totals):
                new = fold(total)
                to = pl.ds(u + n % size, 1)
                if more:
                    new = new + rows_of[n // size, to, :]
                rows_of[n // size, to, :] = new

        pairs = lax.div(v + 1, 2)

        @pl.loop(0, pairs)
        def _(n):
            block(2 * n, 2)

        @pl.when(lax.rem(v, 2) == 0)
        def _():
            block(v, 1)

    def place(which, v):
        change = jnp.zeros((8, 128), jnp.float32)
        turned = jnp.zeros((8, 128), jnp.float32)
        for at, j in which:
            values = jnp.sum(rows_of[at], axis=1, keepdims=True)
            change = change + jnp.where(
                jnp.logical_and(sub <= v, lanes == j * 8 + v), values, 0.0
            )
            turned = turned + jnp.where(
                jnp.logical_and(lanes == j * 8 + sub, sub < v), values, 0.0
            )
        turned = jnp.sum(turned, axis=0, keepdims=True)
        moments[...] = moments[...] + (change + jnp.where(sub == v, turned, 0.0))

    def place_latest(v):
        change = jnp.zeros((8, 128), jnp.float32)
        for at in (0, 1):
            values = jnp.sum(rows_of[at], axis=1, keepdims=True)
            change = change + jnp.where(
                jnp.logical_or(
                    jnp.logical_and(sub <= v, lanes == 16 * sub + (8 * at + v)),
                    jnp.logical_and(sub < v, lanes == 16 * v + 8 * at + sub),
                ),
                values,
                0.0,
            )
        latest[...] = latest[...] + change

    def split(k, part):
        for layer in (0, 1):
            low = pl.multiple_of(TOP + 8 * part, 8)
            values = field[pl.ds(k * BLK, BLK), layer, pl.ds(low, 8), :].reshape(8 * BLK, n_cols)
            high = values.astype(jnp.bfloat16)
            to = pl.ds(pl.multiple_of(k * (8 * BLK), 8 * BLK), 8 * BLK)
            high_ref[layer * tiles + part, to, :] = high
            low_ref[layer * tiles + part, to, :] = (values - high.astype(jnp.float32)).astype(
                jnp.bfloat16
            )

    rows_of[...] = jnp.zeros(rows_of.shape, jnp.float32)

    @pl.loop(0, BLK)
    def _(v):
        load(v).wait()

        send_slow(v)
        send_fast(v)

    @pl.loop(0, BLK)
    def _(v):
        products(v, v, (0,), (0, 1))
        place([(0, 0)], v)

    diag_copy.wait()
    diag[...] = diag[...] + (6.0 - SHIFT)

    def copy(stage, i):
        partner, _, me, base = stage
        return pltpu.make_async_remote_copy(
            src_ref=gathered.at[base + me],
            dst_ref=gathered.at[base + me],
            send_sem=all_send.at[base + i],
            recv_sem=all_recv.at[base + i],
            device_id=partner(i),
            device_id_type=MESH,
        )

    def start(stage, total):
        _, size, me, base = stage
        gathered[base + me] = total
        for i in range(1, size):
            copy(stage, i).start()

    def finish(stage):
        _, size, me, base = stage
        for i in range(1, size):
            copy(stage, i).wait_recv()
        total = gathered[base]
        for i in range(1, size):
            total = total + gathered[base + i]
        return total

    end = (ITERS + 1) * BLK - 1

    def advance(s, k, v):
        others = (k * BLK - BLK, k * BLK)
        arrive_fast(s - BLK)
        apply(s, fast)
        products(s, v, others, (fast,))
        arrive_slow(s - BLK)
        apply(s, core)

        @pl.when(s < ITERS * BLK)
        def _():
            send_slow(s)
            send_fast(s)

        products(s, v, others, (core,), True)

    def advance_last():
        s, v = end, BLK - 1
        others = (s - v - BLK, s - v)
        arrive_fast(s - BLK)
        apply(s, fast)
        products(s, v, others, (fast,))
        apply(s, core, ghost=False)
        products(s, v, others, (core,), True)

        def block(u, holds_last, part):
            totals = [jnp.zeros((8, n_cols), jnp.float32) for _ in range(4)]
            for t in range(part * tiles // 2, (part + 1) * tiles // 2):
                low = TOP + 8 * t
                ghost = low_high[s - BLK, core, 8 * t : 8 * t + 8, :]
                for n in range(4):
                    field_of = field[u + n % 2 + others[n // 2], core, low : low + 8, :]
                    if holds_last and n == 3:
                        field_of = 2.0 * field_of - ghost
                    totals[n] = totals[n] + ghost * field_of
            for n, total in enumerate(totals):
                to = pl.ds(u + n % 2, 1)
                rows_of[n // 2, to, :] = rows_of[n // 2, to, :] - fold(total)

        for part in (0, 1):

            @pl.when(off_chip)
            def _(part=part):
                half_copy(part, fast).wait_recv()

            @pl.loop(0, BLK // 2 - 1)
            def _(n, part=part):
                block(2 * n, False, part)

            block(BLK - 2, True, part)

    @pl.loop(BLK, end)
    def _(s):
        k, v = lax.div(s, BLK), lax.rem(s, BLK)

        @pl.when(s <= BLK + rounds)
        def _():
            r = s - BLK

            @pl.when(r > 0)
            def _():
                pl.semaphore_wait(ready.at[r - 1], partners(*reach(r - 1))[0])

            @pl.when(r < rounds)
            def _():
                tell(ready.at[r], *reach(r))

        @pl.when(s == ITERS * BLK)
        def _():
            start(stages[0], moments[...])

        advance(s, k, v)

        @pl.when(k < ITERS)
        def _():
            place([(0, 2 * k - 1), (1, 2 * k)], v)

        @pl.when(k == ITERS)
        def _():
            place_latest(v)

        split(k - 1, v)

    advance_last()
    place_latest(BLK - 1)

    here = gz * n_gy + gy
    last[here] = jnp.sum(latest[...], axis=0, keepdims=True)
    zs = [around(z_at, i, n_z) * (CORES * Y_CHIPS) for i in range(n_z)]
    ys = [around(y_at, i, Y_CHIPS) * CORES for i in range(Y_CHIPS)]
    xs = [around(gy, i, n_gy) for i in range(n_gy)]
    cores = [core, fast]
    far = lambda i, size: min(i, size - i)
    others = [
        (-(far(a, n_z) + far(b, Y_CHIPS) + far(c, n_gy)), -d, a, b, c)
        for a in range(n_z) for b in range(Y_CHIPS) for c in range(n_gy) for d in range(CORES)
        if a + b + c + d
    ]

    def last_copy(source, device):
        return pltpu.make_async_remote_copy(
            src_ref=source,
            dst_ref=source,
            send_sem=last_send,
            recv_sem=last_recv,
            device_id=device,
            device_id_type=MESH,
        )

    for _, d, a, b, c in sorted(others):
        last_copy(last.at[here], (zs[a] + ys[b] + cores[-d], xs[c])).start()
    start(stages[1], finish(stages[0]))
    split(ITERS - 1, BLK - 1)

    @pl.loop(0, ITERS * BLK - 1)
    def _(s):
        @pl.when(off_chip)
        def _():
            z_copy(s, core, 1).wait_send()

    @pl.when(off_chip)
    def _():
        half_copy(0, core).wait_send()
        half_copy(1, core).wait_send()

    @pl.loop(0, ITERS * BLK // CHUNK)
    def _(n):
        z_copy(n * CHUNK, fast, CHUNK).wait_send()
        for up in (0, 1):

            @pl.when(has_y[up])
            def _(up=up):
                y_copy(n * CHUNK, up).wait_send()

    for stage in stages:
        for i in range(1, stage[1]):
            copy(stage, i).wait_send()
    everyone = last_copy(last.at[pl.ds(0, len(others))], (gz, gy))
    everyone.wait_send()
    total = finish(stages[1])
    x, rows = begin_weights(total)
    everyone.wait_recv()
    sums = [last[i] for i in range(8)]
    for i in range(8, n_gz * n_gy):
        sums[i % 8] = sums[i % 8] + last[i]
    while len(sums) > 1:
        sums = [a + b for a, b in zip(sums[::2], sums[1::2])]
    final = jnp.broadcast_to(sums[0], (8, 128))
    tiles_of = [
        [
            jnp.broadcast_to(
                jnp.sum(
                    jnp.where(lanes == 16 * sub + (8 * at + v), final, 0.0), axis=1, keepdims=True
                ),
                (8, 128),
            )
            for v in range(BLK)
        ]
        for at in (0, 1)
    ]
    for at in (0, 1):
        for v in range(BLK):
            total = jnp.where(lanes == 8 * (2 * ITERS - 1 + at) + v, tiles_of[at][v], total)

    sum_ref[...] = total
    weights = end_weights(x, rows, *tiles_of)
    eighth, within = lax.div(lanes, 8), lax.rem(lanes, 8)
    for i in range(0, BLK, 2):
        wide = []
        for at in (i, i + 1):
            column = [lane(weights[h], at) for h in range(ITERS)]
            front = jnp.where(eighth == sub, column[0], 0.0) + jnp.where(
                eighth == sub + 8, column[1], 0.0
            )
            back = jnp.where(eighth == sub, column[2], 0.0)
            wide.append(
                [
                    jnp.where(within == sub, jnp.sum(part, axis=0, keepdims=True), 0.0)
                    for part in (front, back)
                ]
            )
        for part, (start, stop) in enumerate(((0, 128), (128, 8 * BLK * ITERS))):
            both = jnp.concatenate([wide[0][part], wide[1][part]], axis=0)
            high = both.astype(jnp.bfloat16)
            low = (both - high.astype(jnp.float32)).astype(jnp.bfloat16)
            mix_ref[8 * i : 8 * i + 16, start:stop] = high[:, : stop - start]
            mix_ref[64 + 8 * i : 64 + 8 * i + 16, start:stop] = low[:, : stop - start]


def combine(high_ref, low_ref, mix_ref, sum_ref, out_ref, hess_ref, result, hess, out_sem, hess_sem):
    tiles = high_ref.shape[0] // 2

    def store(n):
        where = (slice(None), n // tiles, pl.ds(8 * (n % tiles), 8))
        return pltpu.make_async_copy(result.at[where], out_ref.at[where], out_sem.at[n])

    for h, tile in enumerate(hessenberg_of(sum_ref[...])):
        hess[8 * h : 8 * h + 8, :] = tile[:, : hess.shape[1]]
    for n in range(2 * tiles):
        both = jnp.dot(mix_ref[...], high_ref[n], preferred_element_type=jnp.float32)
        rest = jnp.dot(mix_ref[:64], low_ref[n], preferred_element_type=jnp.float32)
        total = both[:64] + (both[64:] + rest)
        result[:, n // tiles, 8 * (n % tiles) : 8 * (n % tiles) + 8, :] = total.reshape(
            BLK, 8, total.shape[1]
        )
        store(n).start()
    copy = pltpu.make_async_copy(hess, hess_ref, hess_sem)
    copy.start()
    for n in range(2 * tiles):
        store(n).wait()
    copy.wait()


def solution(mesh):
    n_gz, n_gy = mesh.shape["gz"], mesh.shape["gy"]
    n_z = n_gz // (CORES * Y_CHIPS)
    partners = n_gy * Y_CHIPS + n_z * CORES

    def body(right_side, diagonal):
        layers, n_rows, n_cols = diagonal.shape
        powers = ITERS * BLK
        pieces = layers * n_rows // 8
        vmem = lambda *shape: pltpu.VMEM(shape, jnp.float32)
        dma = pltpu.SemaphoreType.DMA
        whole = pl.BlockSpec(memory_space=pltpu.VMEM)
        high, low, mix, moments = pl.pallas_call(
            functools.partial(kernel, n_gz, n_gy),
            out_shape=(
                jax.ShapeDtypeStruct((pieces, 8 * powers, n_cols), jnp.bfloat16),
                jax.ShapeDtypeStruct((pieces, 8 * powers, n_cols), jnp.bfloat16),
                jax.ShapeDtypeStruct((16 * BLK, 8 * powers), jnp.bfloat16),
                jax.ShapeDtypeStruct((8, 128), jnp.float32),
            ),
            in_specs=[pl.BlockSpec(memory_space=pltpu.HBM)] * 2,
            out_specs=(whole,) * 4,
            scratch_shapes=[
                vmem(powers + BLK, layers, n_rows + 2 * TOP, n_cols),
                vmem(powers, 2, n_rows, n_cols),
                vmem(2, powers, layers, 1, n_cols),
                vmem(2, powers, layers, 1, n_cols),
                vmem(layers, n_rows, n_cols),
                vmem(2, 8, 128),
                vmem(8, 128),
                vmem(8, 128),
                vmem(partners, 8, 128),
                vmem(n_gz * n_gy, 1, 128),
                dma((BLK,)),
                dma,
                dma((powers + 1, 2)),
                dma((powers + 1, 2)),
                dma((powers, 2)),
                dma((powers, 2)),
                dma((partners,)),
                dma((partners,)),
                pltpu.SemaphoreType.REGULAR((16,)),
                dma,
                dma,
            ],
            compiler_params=pltpu.CompilerParams(
                collective_id=0, has_side_effects=True, vmem_limit_bytes=28 << 20
            ),
            name="block_gmres",
        )(*(pltpu.with_memory_space_constraint(a, pltpu.HBM) for a in (right_side, diagonal)))
        return pl.pallas_call(
            combine,
            out_shape=(
                jax.ShapeDtypeStruct(right_side.shape, jnp.float32),
                jax.ShapeDtypeStruct((powers, powers + BLK), jnp.float32),
            ),
            in_specs=[whole] * 4,
            out_specs=(pl.BlockSpec(memory_space=pltpu.HBM),) * 2,
            scratch_shapes=[
                vmem(*right_side.shape),
                vmem(powers, powers + BLK),
                dma((pieces,)),
                dma,
            ],
            compiler_params=pltpu.CompilerParams(vmem_limit_bytes=12 << 20),
            name="combine",
        )(high, low, mix, moments)

    placed = (P(None, "gz", "gy", None), P("gz", "gy", None))
    return jax.shard_map(
        body, mesh=mesh, in_specs=placed, out_specs=(placed[0], P()), check_vma=False
    )
```

```python
import functools

import jax
import jax.numpy as jnp
from jax import lax
from jax.experimental import pallas as pl
from jax.experimental.pallas import tpu as pltpu
from jax.sharding import PartitionSpec as P

MESH = pl.DeviceIdType.MESH
BLK = 8
ITERS = 3
SHIFT = 7.0
TOP = 8
Y_CHIPS = 4
CORES = 2
CHUNK = 4


def iotas():
    return (
        lax.broadcasted_iota(jnp.int32, (8, 128), 0),
        lax.broadcasted_iota(jnp.int32, (8, 128), 1),
    )


def sublane(tile, at):
    return jnp.broadcast_to(tile[at : at + 1, :], (8, 128))


def lane(tile, at):
    return jnp.broadcast_to(tile[:, at : at + 1], (8, 128))


def rsqrt(value):
    guess = lax.rsqrt(value)
    return guess * (1.5 - 0.5 * value * guess * guess)


def eliminate(x, rows, start, stop):
    sub, _ = iotas()
    for k in range(start, stop):
        g, q = divmod(k, 8)
        column = rows[k]
        inverse = 1.0 / sublane(column[g], q)
        pivot = sublane(x[g], q) * inverse
        for h in range(ITERS):
            x[h] = x[h] - column[h] * pivot
        x[g] = jnp.where(sub == q, pivot, x[g])
        for r in range(k + 1, len(rows)):
            factor = sublane(column[r // 8], r % 8) * inverse
            rows[r] = [rows[r][h] - factor * column[h] for h in range(ITERS)]
            rows[r][g] = jnp.where(sub == q, factor, rows[r][g])


def begin_weights(moments):
    one = pltpu.roll(moments, 128 - 8, 1)
    two = pltpu.roll(moments, 128 - 16, 1)
    squares = two + (2.0 * SHIFT) * one + (SHIFT * SHIFT) * moments
    right = one + SHIFT * moments
    x = [right if h == 0 else pltpu.roll(right, 128 - 8 * h, 1) for h in range(ITERS)]
    tiles = [[lane(squares, 8 * j + v) for v in range(8)] for j in range(2 * ITERS - 1)]
    rows = [[tiles[a + h][i] for h in range(ITERS)] for a in range(ITERS) for i in range(8)]
    eliminate(x, rows, 0, 8)
    return x, rows


def end_weights(x, rows, fifth, sixth):
    for v in range(8):
        rows[8 + v][2] = rows[8 + v][2] + fifth[v]
        rows[16 + v][1] = rows[16 + v][1] + fifth[v]
        rows[16 + v][2] = rows[16 + v][2] + (sixth[v] + (2.0 * SHIFT) * fifth[v])
    eliminate(x, rows, 8, 8 * ITERS)
    return x


def hessenberg_of(moments):
    sub, lanes = iotas()
    tiles = [[lane(moments, 8 * j + v) for v in range(8)] for j in range(2 * ITERS + 1)]
    groups = ITERS + 1
    rows = [[tiles[a + h][i] for h in range(groups)] for a in range(groups) for i in range(8)]
    size = 8 * groups
    factor_of, scale_of = [], []
    for k in range(size):
        g, q = divmod(k, 8)
        scale = rsqrt(sublane(rows[k][g], q))
        column = [None if h < g else rows[k][h] * scale for h in range(groups)]
        column[g] = jnp.where(sub >= q, column[g], 0.0)
        factor_of.append(column)
        scale_of.append(scale)
        for r in range(k + 1, size):
            factor = sublane(column[r // 8], r % 8)
            for h in range(r // 8, groups):
                rows[r][h] = rows[r][h] - factor * column[h]
    x = []
    for h in range(ITERS):
        tile = jnp.zeros((8, 128), jnp.float32)
        for c in range(8 * (h + 2)):
            tile = jnp.where(lanes == c, factor_of[c][h + 1], tile)
        x.append(tile)
    for k in range(8 * ITERS):
        g, q = divmod(k, 8)
        solved = sublane(x[g], q) * scale_of[k]
        for h in range(g, ITERS):
            x[h] = x[h] - factor_of[k][h] * solved
        x[g] = jnp.where(sub == q, solved, x[g])
    return [x[h] + jnp.where(lanes == 8 * h + sub, SHIFT, 0.0) for h in range(ITERS)]


def kernel(
    n_gz, n_gy, b_ref, d_ref, high_ref, low_ref, mix_ref, sum_ref,
    field, low_high, side_in, side_out, diag, rows_of, moments, latest, gathered, last,
    load_sem, diag_sem, z_send, z_recv, y_send, y_recv, all_send, all_recv, ready, last_send, last_recv,
):
    gz, gy = lax.axis_index("gz"), lax.axis_index("gy")
    n_rows, n_cols = d_ref.shape[1], d_ref.shape[2]
    tiles = n_rows // 8
    core = lax.rem(gz, CORES)
    y_at = lax.rem(lax.div(gz, CORES), Y_CHIPS)
    z_at = lax.div(gz, CORES * Y_CHIPS)
    n_z = n_gz // (CORES * Y_CHIPS)
    fast = 1 - core
    own = pl.ds(TOP, n_rows)
    sub, lanes = iotas()

    def partners(gz_step, gy_step):
        both = []
        for sign in (-1, 1):
            to_gz, to_gy = gz + sign * gz_step, gy + sign * gy_step
            there = jnp.logical_and(
                jnp.logical_and(to_gz >= 0, to_gz < n_gz), jnp.logical_and(to_gy >= 0, to_gy < n_gy)
            )
            both.append((there, (to_gz, to_gy)))
        return sum(jnp.where(there, 1, 0) for there, _ in both), both

    def tell(semaphore, gz_step, gy_step):
        count, both = partners(gz_step, gy_step)
        for there, device in both:

            @pl.when(there)
            def _(device=device):
                pl.semaphore_signal(semaphore, inc=1, device_id=device, device_id_type=MESH)

        return count

    barrier = pltpu.get_barrier_semaphore()
    expected = tell(barrier, 1, 0) + tell(barrier, 0, 1)

    def load(v):
        return pltpu.make_async_copy(b_ref.at[v], field.at[v, :, own, :], load_sem.at[v])

    diag_copy = pltpu.make_async_copy(d_ref, diag, diag_sem)
    load(0).start()
    load(1).start()
    diag_copy.start()
    for v in range(2, BLK):
        load(v).start()

    def around(at, i, size):
        return at + i if i == 0 else jnp.where(at + i >= size, at + (i - size), at + i)

    def over_yx(i):
        return (gz + (around(y_at, i // n_gy, Y_CHIPS) - y_at) * CORES, around(gy, i % n_gy, n_gy))

    def over_zc(i):
        to = (around(z_at, i // CORES, n_z) - z_at) * CORES * Y_CHIPS
        return (gz + to + around(core, i % CORES, CORES) - core, gy)

    stages = (
        (over_zc, n_z * CORES, z_at * CORES + core, Y_CHIPS * n_gy),
        (over_yx, Y_CHIPS * n_gy, y_at * n_gy + gy, 0),
    )

    def clear(where, at):
        @pl.when(where)
        def _():
            @pl.loop(0, ITERS * BLK)
            def _(s):
                buffer = at(s)
                buffer[...] = jnp.zeros(buffer.shape, jnp.float32)

    for side, z_edge, y_edge in ((0, 0, 0), (1, n_gz - 1, n_gy - 1)):
        clear(gz == z_edge, lambda s, side=side: low_high.at[s, side])
        clear(gy == y_edge, lambda s, side=side: side_in.at[side, s])
    moments[...] = jnp.zeros((8, 128), jnp.float32)
    latest[...] = jnp.zeros((8, 128), jnp.float32)

    off_chip = jnp.where(core == 0, gz > 0, gz < n_gz - 1)

    pl.semaphore_wait(barrier, expected)

    doublings = (n_gz - 1).bit_length()
    rounds = doublings + n_gy - 1

    def reach(r):
        gz_step = 1
        for i in range(1, doublings):
            gz_step = jnp.where(r == i, 2**i, gz_step)
        along_gz = r < doublings
        return jnp.where(along_gz, gz_step, 0), jnp.where(along_gz, 0, 1)

    def z_copy(s, up, size):
        return pltpu.make_async_remote_copy(
            src_ref=field.at[pl.ds(s, size), up, own, :],
            dst_ref=low_high.at[pl.ds(s, size), 1 - up],
            send_sem=z_send.at[s, up],
            recv_sem=z_recv.at[s, 1 - up],
            device_id=(gz + 2 * up - 1, gy),
            device_id_type=MESH,
        )

    def by_chunk(s, at_end, do):
        edge = CHUNK - 1 if at_end else 0
        if isinstance(s, int):
            if s < ITERS * BLK and s % CHUNK == edge:
                do(s - edge)
            return

        @pl.when(jnp.logical_and(s < ITERS * BLK, lax.rem(s, CHUNK) == edge))
        def _():
            do(s - edge)

    def y_copy(s, up):
        return pltpu.make_async_remote_copy(
            src_ref=side_out.at[up, pl.ds(s, CHUNK)],
            dst_ref=side_in.at[1 - up, pl.ds(s, CHUNK)],
            send_sem=y_send.at[s, up],
            recv_sem=y_recv.at[s, 1 - up],
            device_id=(gz, gy + 2 * up - 1),
            device_id_type=MESH,
        )

    has_y = (gy > 0, gy < n_gy - 1)

    def send_slow(s):
        @pl.when(off_chip)
        def _():
            z_copy(s, core, 1).start()

    def send_fast(s):
        for layer in (0, 1):
            side_out[0, s, layer] = field[s, layer, TOP : TOP + 1, :]
            side_out[1, s, layer] = field[s, layer, TOP + n_rows - 1 : TOP + n_rows, :]

        def start(at):
            z_copy(at, fast, CHUNK).start()
            for up in (0, 1):

                @pl.when(has_y[up])
                def _(up=up):
                    y_copy(at, up).start()

        by_chunk(s, True, start)

    def arrive_fast(s):
        def wait(at):
            z_copy(at, core, CHUNK).wait_recv()
            for up in (0, 1):

                @pl.when(has_y[up])
                def _(up=up):
                    y_copy(at, 1 - up).wait_recv()

        by_chunk(s, False, wait)
        for layer in (0, 1):
            field[s, layer, TOP - 1 : TOP, :] = side_in[0, s, layer]
            field[s, layer, TOP + n_rows : TOP + n_rows + 1, :] = side_in[1, s, layer]

    def arrive_slow(s):
        @pl.when(off_chip)
        def _():
            z_copy(s, fast, 1).wait_recv()

    lane_of_row = lax.broadcasted_iota(jnp.int32, (8, n_cols), 1)

    def apply(s, layer, ghost=True):
        f = s - BLK
        for t in range(tiles):
            low = TOP + 8 * t
            here = field[f, layer, low : low + 8, :]
            beside = field[f, layer, low - 1 : low + 7, :] + field[f, layer, low + 1 : low + 9, :]
            other = field[f, 1 - layer, low : low + 8, :]
            if ghost:
                other = other + low_high[f, layer, 8 * t : 8 * t + 8, :]
            beside = beside + other
            left = jnp.where(lane_of_row == 0, 0.0, pltpu.roll(here, 1, 1))
            right = jnp.where(lane_of_row == n_cols - 1, 0.0, pltpu.roll(here, n_cols - 1, 1))
            field[s, layer, low : low + 8, :] = diag[layer, 8 * t : 8 * t + 8, :] * here - (
                beside + (left + right)
            )

    def fold(row):
        total = row[:, :128]
        for at in range(128, n_cols, 128):
            total = total + row[:, at : at + 128]
        return jnp.sum(total, axis=0, keepdims=True)

    def products(s, v, others, layers, more=False):
        def block(u, size):
            totals = [jnp.zeros((8, n_cols), jnp.float32) for _ in range(size * len(others))]
            for layer in layers:
                for t in range(tiles):
                    low = TOP + 8 * t
                    here = field[s, layer, low : low + 8, :]
                    totals = [
                        total + here * field[u + n % size + others[n // size], layer, low : low + 8, :]
                        for n, total in enumerate(totals)
                    ]
            for n, total in enumerate(totals):
                new = fold(total)
                to = pl.ds(u + n % size, 1)
                if more:
                    new = new + rows_of[n // size, to, :]
                rows_of[n // size, to, :] = new

        pairs = lax.div(v + 1, 2)

        @pl.loop(0, pairs)
        def _(n):
            block(2 * n, 2)

        @pl.when(lax.rem(v, 2) == 0)
        def _():
            block(v, 1)

    def place(which, v):
        change = jnp.zeros((8, 128), jnp.float32)
        turned = jnp.zeros((8, 128), jnp.float32)
        for at, j in which:
            values = jnp.sum(rows_of[at], axis=1, keepdims=True)
            change = change + jnp.where(
                jnp.logical_and(sub <= v, lanes == j * 8 + v), values, 0.0
            )
            turned = turned + jnp.where(
                jnp.logical_and(lanes == j * 8 + sub, sub < v), values, 0.0
            )
        turned = jnp.sum(turned, axis=0, keepdims=True)
        moments[...] = moments[...] + (change + jnp.where(sub == v, turned, 0.0))

    def place_latest(v):
        change = jnp.zeros((8, 128), jnp.float32)
        for at in (0, 1):
            values = jnp.sum(rows_of[at], axis=1, keepdims=True)
            change = change + jnp.where(
                jnp.logical_or(
                    jnp.logical_and(sub <= v, lanes == 16 * sub + (8 * at + v)),
                    jnp.logical_and(sub < v, lanes == 16 * v + 8 * at + sub),
                ),
                values,
                0.0,
            )
        latest[...] = latest[...] + change

    def split(k, part):
        for layer in (0, 1):
            low = pl.multiple_of(TOP + 8 * part, 8)
            values = field[pl.ds(k * BLK, BLK), layer, pl.ds(low, 8), :].reshape(8 * BLK, n_cols)
            high = values.astype(jnp.bfloat16)
            to = pl.ds(pl.multiple_of(k * (8 * BLK), 8 * BLK), 8 * BLK)
            high_ref[layer * tiles + part, to, :] = high
            low_ref[layer * tiles + part, to, :] = (values - high.astype(jnp.float32)).astype(
                jnp.bfloat16
            )

    rows_of[...] = jnp.zeros(rows_of.shape, jnp.float32)

    @pl.loop(0, BLK)
    def _(v):
        load(v).wait()

        send_slow(v)
        send_fast(v)

    @pl.loop(0, BLK)
    def _(v):
        products(v, v, (0,), (0, 1))
        place([(0, 0)], v)

    diag_copy.wait()
    diag[...] = diag[...] + (6.0 - SHIFT)

    def copy(stage, i):
        partner, _, me, base = stage
        return pltpu.make_async_remote_copy(
            src_ref=gathered.at[base + me],
            dst_ref=gathered.at[base + me],
            send_sem=all_send.at[base + i],
            recv_sem=all_recv.at[base + i],
            device_id=partner(i),
            device_id_type=MESH,
        )

    def start(stage, total):
        _, size, me, base = stage
        gathered[base + me] = total
        for i in range(1, size):
            copy(stage, i).start()

    def finish(stage):
        _, size, me, base = stage
        for i in range(1, size):
            copy(stage, i).wait_recv()
        total = gathered[base]
        for i in range(1, size):
            total = total + gathered[base + i]
        return total

    end = (ITERS + 1) * BLK - 1

    def advance(s, k, v):
        others = (k * BLK - BLK, k * BLK)
        arrive_fast(s - BLK)
        apply(s, fast)
        products(s, v, others, (fast,))
        arrive_slow(s - BLK)
        apply(s, core)

        @pl.when(s < ITERS * BLK)
        def _():
            send_slow(s)
            send_fast(s)

        products(s, v, others, (core,), True)

    def advance_last():
        s, v = end, BLK - 1
        others = (s - v - BLK, s - v)
        arrive_fast(s - BLK)
        apply(s, fast)
        products(s, v, others, (fast,))
        apply(s, core, ghost=False)
        products(s, v, others, (core,), True)
        arrive_slow(s - BLK)

        def block(u, holds_last):
            totals = [jnp.zeros((8, n_cols), jnp.float32) for _ in range(4)]
            for t in range(tiles):
                low = TOP + 8 * t
                ghost = low_high[s - BLK, core, 8 * t : 8 * t + 8, :]
                for n in range(4):
                    field_of = field[u + n % 2 + others[n // 2], core, low : low + 8, :]
                    if holds_last and n == 3:
                        field_of = 2.0 * field_of - ghost
                    totals[n] = totals[n] + ghost * field_of
            for n, total in enumerate(totals):
                to = pl.ds(u + n % 2, 1)
                rows_of[n // 2, to, :] = rows_of[n // 2, to, :] - fold(total)

        @pl.loop(0, BLK // 2 - 1)
        def _(n):
            block(2 * n, False)

        block(BLK - 2, True)

    @pl.loop(BLK, end)
    def _(s):
        k, v = lax.div(s, BLK), lax.rem(s, BLK)

        @pl.when(jnp.logical_and(s <= BLK + 2 * rounds, lax.rem(s - BLK, 2) == 0))
        def _():
            r = lax.div(s - BLK, 2)

            @pl.when(r > 0)
            def _():
                pl.semaphore_wait(ready.at[r - 1], partners(*reach(r - 1))[0])

            @pl.when(r < rounds)
            def _():
                tell(ready.at[r], *reach(r))

        @pl.when(s == ITERS * BLK)
        def _():
            start(stages[0], moments[...])

        advance(s, k, v)

        @pl.when(k < ITERS)
        def _():
            place([(0, 2 * k - 1), (1, 2 * k)], v)

        @pl.when(k == ITERS)
        def _():
            place_latest(v)

        split(k - 1, v)

    advance_last()
    place_latest(BLK - 1)

    here = gz * n_gy + gy
    last[here] = jnp.sum(latest[...], axis=0, keepdims=True)
    zs = [around(z_at, i, n_z) * (CORES * Y_CHIPS) for i in range(n_z)]
    ys = [around(y_at, i, Y_CHIPS) * CORES for i in range(Y_CHIPS)]
    xs = [around(gy, i, n_gy) for i in range(n_gy)]
    cores = [core, fast]
    far = lambda i, size: min(i, size - i)
    others = [
        (-(far(a, n_z) + far(b, Y_CHIPS) + far(c, n_gy)), -d, a, b, c)
        for a in range(n_z) for b in range(Y_CHIPS) for c in range(n_gy) for d in range(CORES)
        if a + b + c + d
    ]

    def last_copy(source, device):
        return pltpu.make_async_remote_copy(
            src_ref=source,
            dst_ref=source,
            send_sem=last_send,
            recv_sem=last_recv,
            device_id=device,
            device_id_type=MESH,
        )

    for _, d, a, b, c in sorted(others):
        last_copy(last.at[here], (zs[a] + ys[b] + cores[-d], xs[c])).start()
    start(stages[1], finish(stages[0]))
    split(ITERS - 1, BLK - 1)

    @pl.loop(0, ITERS * BLK)
    def _(s):
        @pl.when(off_chip)
        def _():
            z_copy(s, core, 1).wait_send()

    @pl.loop(0, ITERS * BLK // CHUNK)
    def _(n):
        z_copy(n * CHUNK, fast, CHUNK).wait_send()
        for up in (0, 1):

            @pl.when(has_y[up])
            def _(up=up):
                y_copy(n * CHUNK, up).wait_send()

    for stage in stages:
        for i in range(1, stage[1]):
            copy(stage, i).wait_send()
    everyone = last_copy(last.at[pl.ds(0, len(others))], (gz, gy))
    everyone.wait_send()
    total = finish(stages[1])
    x, rows = begin_weights(total)
    everyone.wait_recv()
    sums = [last[i] for i in range(8)]
    for i in range(8, n_gz * n_gy):
        sums[i % 8] = sums[i % 8] + last[i]
    while len(sums) > 1:
        sums = [a + b for a, b in zip(sums[::2], sums[1::2])]
    final = jnp.broadcast_to(sums[0], (8, 128))
    tiles_of = [
        [
            jnp.broadcast_to(
                jnp.sum(
                    jnp.where(lanes == 16 * sub + (8 * at + v), final, 0.0), axis=1, keepdims=True
                ),
                (8, 128),
            )
            for v in range(BLK)
        ]
        for at in (0, 1)
    ]
    for at in (0, 1):
        for v in range(BLK):
            total = jnp.where(lanes == 8 * (2 * ITERS - 1 + at) + v, tiles_of[at][v], total)

    sum_ref[...] = total
    weights = end_weights(x, rows, *tiles_of)
    eighth, within = lax.div(lanes, 8), lax.rem(lanes, 8)
    for i in range(0, BLK, 2):
        wide = []
        for at in (i, i + 1):
            column = [lane(weights[h], at) for h in range(ITERS)]
            front = jnp.where(eighth == sub, column[0], 0.0) + jnp.where(
                eighth == sub + 8, column[1], 0.0
            )
            back = jnp.where(eighth == sub, column[2], 0.0)
            wide.append(
                [
                    jnp.where(within == sub, jnp.sum(part, axis=0, keepdims=True), 0.0)
                    for part in (front, back)
                ]
            )
        for part, (start, stop) in enumerate(((0, 128), (128, 8 * BLK * ITERS))):
            both = jnp.concatenate([wide[0][part], wide[1][part]], axis=0)
            high = both.astype(jnp.bfloat16)
            low = (both - high.astype(jnp.float32)).astype(jnp.bfloat16)
            mix_ref[8 * i : 8 * i + 16, start:stop] = high[:, : stop - start]
            mix_ref[64 + 8 * i : 64 + 8 * i + 16, start:stop] = low[:, : stop - start]


def combine(high_ref, low_ref, mix_ref, sum_ref, out_ref, hess_ref, result, hess, out_sem, hess_sem):
    tiles = high_ref.shape[0] // 2

    def store(n):
        where = (slice(None), n // tiles, pl.ds(8 * (n % tiles), 8))
        return pltpu.make_async_copy(result.at[where], out_ref.at[where], out_sem.at[n])

    for h, tile in enumerate(hessenberg_of(sum_ref[...])):
        hess[8 * h : 8 * h + 8, :] = tile[:, : hess.shape[1]]
    for n in range(2 * tiles):
        both = jnp.dot(mix_ref[...], high_ref[n], preferred_element_type=jnp.float32)
        rest = jnp.dot(mix_ref[:64], low_ref[n], preferred_element_type=jnp.float32)
        total = both[:64] + (both[64:] + rest)
        result[:, n // tiles, 8 * (n % tiles) : 8 * (n % tiles) + 8, :] = total.reshape(
            BLK, 8, total.shape[1]
        )
        store(n).start()
    copy = pltpu.make_async_copy(hess, hess_ref, hess_sem)
    copy.start()
    for n in range(2 * tiles):
        store(n).wait()
    copy.wait()


def solution(mesh):
    n_gz, n_gy = mesh.shape["gz"], mesh.shape["gy"]
    n_z = n_gz // (CORES * Y_CHIPS)
    partners = n_gy * Y_CHIPS + n_z * CORES

    def body(right_side, diagonal):
        layers, n_rows, n_cols = diagonal.shape
        powers = ITERS * BLK
        pieces = layers * n_rows // 8
        vmem = lambda *shape: pltpu.VMEM(shape, jnp.float32)
        dma = pltpu.SemaphoreType.DMA
        whole = pl.BlockSpec(memory_space=pltpu.VMEM)
        high, low, mix, moments = pl.pallas_call(
            functools.partial(kernel, n_gz, n_gy),
            out_shape=(
                jax.ShapeDtypeStruct((pieces, 8 * powers, n_cols), jnp.bfloat16),
                jax.ShapeDtypeStruct((pieces, 8 * powers, n_cols), jnp.bfloat16),
                jax.ShapeDtypeStruct((16 * BLK, 8 * powers), jnp.bfloat16),
                jax.ShapeDtypeStruct((8, 128), jnp.float32),
            ),
            in_specs=[pl.BlockSpec(memory_space=pltpu.HBM)] * 2,
            out_specs=(whole,) * 4,
            scratch_shapes=[
                vmem(powers + BLK, layers, n_rows + 2 * TOP, n_cols),
                vmem(powers, 2, n_rows, n_cols),
                vmem(2, powers, layers, 1, n_cols),
                vmem(2, powers, layers, 1, n_cols),
                vmem(layers, n_rows, n_cols),
                vmem(2, 8, 128),
                vmem(8, 128),
                vmem(8, 128),
                vmem(partners, 8, 128),
                vmem(n_gz * n_gy, 1, 128),
                dma((BLK,)),
                dma,
                dma((powers, 2)),
                dma((powers, 2)),
                dma((powers, 2)),
                dma((powers, 2)),
                dma((partners,)),
                dma((partners,)),
                pltpu.SemaphoreType.REGULAR((16,)),
                dma,
                dma,
            ],
            compiler_params=pltpu.CompilerParams(
                collective_id=0, has_side_effects=True, vmem_limit_bytes=28 << 20
            ),
            name="block_gmres",
        )(*(pltpu.with_memory_space_constraint(a, pltpu.HBM) for a in (right_side, diagonal)))
        return pl.pallas_call(
            combine,
            out_shape=(
                jax.ShapeDtypeStruct(right_side.shape, jnp.float32),
                jax.ShapeDtypeStruct((powers, powers + BLK), jnp.float32),
            ),
            in_specs=[whole] * 4,
            out_specs=(pl.BlockSpec(memory_space=pltpu.HBM),) * 2,
            scratch_shapes=[
                vmem(*right_side.shape),
                vmem(powers, powers + BLK),
                dma((pieces,)),
                dma,
            ],
            compiler_params=pltpu.CompilerParams(vmem_limit_bytes=12 << 20),
            name="combine",
        )(high, low, mix, moments)

    placed = (P(None, "gz", "gy", None), P("gz", "gy", None))
    return jax.shard_map(
        body, mesh=mesh, in_specs=placed, out_specs=(placed[0], P()), check_vma=False
    )
```
